256 devices in a mesh: dp: 2 (over core), expert: 8 (over z), ffn: 16 (over y, x).
Axes of the slice: x: 4, y: 4, z: 8, core: 2. Of those that a mesh axis runs over, the one named last changes fastest.
Arguments:
- tokens: bfloat16 [2048, 6144], P(('dp', 'expert'), 'ffn'), may hold values from -6 to 6
- routes: int32 [2048, 2], P(('dp', 'expert')), may hold values from 0 to 7, all different within a row; in each aligned block of 128 rows (0 to 127, 128 to 255, ...) at most 64 rows name the same one
- keep: int32 [16, 8], P(('dp', 'expert')), may hold values from 0 to 1, as said below
- router: float32 [6144, 8], P('ffn'), may hold values from -0.078125 to 0.078125
- w_gate: bfloat16 [8, 6144, 8192], P('expert', None, ('dp', 'ffn')), may hold values from -0.078125 to 0.078125
- w_up: bfloat16 [8, 6144, 8192], P('expert', None, ('dp', 'ffn')), may hold values from -0.078125 to 0.078125
- w_down: bfloat16 [8, 8192, 6144], P('expert', ('dp', 'ffn')), may hold values from -0.125 to 0.125
Outputs:
- full_out: bfloat16 [2048, 6144], P(('dp', 'expert'), 'ffn')
- pruned_out: bfloat16 [2048, 6144], P(('dp', 'expert'), 'ffn')
- residual: float32 [2048, 6144], P(('dp', 'expert'), 'ffn')
- router_grad: float32 [6144, 8], P('ffn')
The draws below stay inside these ranges and needn't reach their ends.
Inputs may be any that keep to these rules, and one draw needn't show every extreme that they name: `routes`: each row names two different experts; in the 128 rows of one block no expert is named by more than 64 rows, a bound that some block reaches. `keep`: in every row between 2 and 4 entries are 0, the others 1.
All inputs are finite; a program needn't handle non-finite values.
Results may differ from the reference program's by a relative error of at most 0.02.
Values may be sent and summed in bfloat16 or wider, within the bound.
A program may use at most 128 MiB of HBM per device.

```python
import math
import jax
import jax.numpy as jnp
import numpy as np
from jax import lax

D = 6144
FFW = 8192
TOK_DEV = 128
EXPERTS = 8
CAP = 64
DROP = 2
BLOCKS = 16
TOKENS = 2048
N_DP = 2
N_EXPERT = 8
N_FFN = 16


def draw_keep(key, part):

    def one_block(index):
        block_key = jax.random.fold_in(key, 101 + index)
        order = jax.random.permutation(jax.random.fold_in(block_key, 11), EXPERTS)
        dropped = jax.random.randint(jax.random.fold_in(block_key, 23), (), DROP, 2 * DROP + 1)
        return (order >= dropped).astype(jnp.int32)
    return jax.vmap(one_block)(jnp.arange(BLOCKS, dtype=jnp.int32))


def with_spikes(values, own_key, source, target, blocks, factor):
    def block_of(axis_at):
        return (jnp.arange(values.shape[axis_at]) // (values.shape[axis_at] // blocks)).reshape((-1,) + (1,) * (values.ndim - 1 - axis_at))

    first = jax.random.permutation(own_key, blocks)[block_of(target)]
    far = (block_of(target) + blocks // 2) % blocks
    return jnp.where((block_of(source) == first) | (block_of(source) == far), factor * values, values)


def levels(own_key, dims, shards, least, top_value):
    def one(position, shards_of):
        draws = jax.random.uniform(jax.random.fold_in(jax.random.fold_in(own_key, 6), position), (shards_of,), jnp.float32, least / len(shards), top_value / len(shards))
        return jnp.repeat(jnp.exp(draws), dims[position] // shards_of).reshape((-1,) + (1,) * (len(dims) - position - 1))

    factor_of = one(*shards[0])
    for cut in shards[1:]:
        factor_of = factor_of * one(*cut)
    return factor_of


def routed_block(own_key, own, number, rows, amount, top, reach, lean):
    order = jax.random.permutation(own_key, amount)
    packed, usual = portions_of(amount, rows * top, reach, lean, True), portions_of(amount, rows * top, reach, lean, False)
    places = jnp.arange(amount)

    def named(tallies, turn):
        used = int((tallies > 0).sum())
        fixed = max(1, used // 4)
        shifted = fixed + (places - fixed + turn * (used - fixed)) % max(1, amount - fixed)
        return jnp.zeros((amount,), jnp.int32).at[order[jnp.where(places < fixed, places, shifted)]].set(jnp.asarray(tallies, jnp.int32))

    tallies = jnp.where(number % 4 == 0, named(packed, number // 4), named(usual, number - number // 4 - 1))
    mixed = jax.random.permutation(jax.random.fold_in(own, 3), amount)
    donor, sink = mixed[0:amount // 2 * 2:2], mixed[1:amount // 2 * 2:2]
    room = jnp.minimum(tallies[donor] - 1, reach - tallies[sink]) // 2
    room = jnp.where((donor == order[0]) | (sink == order[0]) | (tallies[sink] == 0), 0, jnp.maximum(room, 0))
    shifted = jax.random.randint(jax.random.fold_in(own, 4), (amount // 2,), 0, 1 << 20) % (room + 1)
    tallies = tallies.at[donor].add(-shifted).at[sink].add(shifted)
    items = jnp.searchsorted(jnp.cumsum(tallies), jnp.arange(rows * top), side="right").astype(jnp.int32)
    listing = items.reshape(top, rows).T
    listing = listing[jax.random.permutation(jax.random.fold_in(own, 1), rows)]
    turn = jax.random.randint(jax.random.fold_in(own, 2), (rows, 1), 0, top)
    return jnp.take_along_axis(listing, (jnp.arange(top)[None, :] + turn) % top, axis=1)


def portions_of(count, total, reach, skew, full):
    loads = [(1 << 20) // math.isqrt(grade ** skew) + 1 for grade in range(1, count + 1)]
    largest = reach if full else min(reach, max(-(-total // count), total * loads[0] // sum(loads)))
    least = 1 if total - largest >= count - 1 else 0
    given, spare = [largest] + [least] * (count - 1), total - largest - least * (count - 1)
    while spare > 0:
        movable = [i for i in range(1, count) if given[i] < largest] or [i for i in range(1, count) if given[i] < reach]
        mass, left = sum([loads[i] for i in movable]), spare
        for i in movable:
            more = min(reach - given[i], max(1, left * loads[i] // mass), spare)
            given[i] = given[i] + more
            spare = spare - more
    return np.array(given)


def bell_draw(rng, extent, scale, most, shards=(), held_as=jnp.bfloat16):
    entries = jax.random.normal(rng, extent, jnp.float32) * scale
    if len(shards) > 0:
        entries = levels(rng, extent, shards, -0.22, 0.18) * entries
    return jnp.clip(entries, min=-most, max=most).astype(held_as)


def gaussian_with(stream_key, extent, scale, reach, cuts, heavy, held_as=jnp.bfloat16):
    result = scale * jax.random.normal(stream_key, extent, jnp.float32)
    if cuts:
        result = result * levels(stream_key, extent, cuts, -0.22, 0.18)
    return jnp.clip(with_spikes(result, jax.random.fold_in(stream_key, 3), *heavy), -reach, reach).astype(held_as)


def setup_inputs(seed: int = 0) -> dict:
    splits = jax.random.split(jax.random.key(seed), 8)
    tokens = bell_draw(splits[0], (TOKENS, D), 1.0, 6.0, ((0, 16), (1, 16)))
    routes_keys = jax.random.split(jax.random.fold_in(splits[1], 1), TOKENS // TOK_DEV)
    routes_turns = jax.random.permutation(jax.random.fold_in(splits[1], 3), TOKENS // TOK_DEV)
    routes = jax.vmap(lambda own, number: routed_block(jax.random.fold_in(splits[1], 2), own, number, TOK_DEV, EXPERTS, 2, CAP, 1))(routes_keys, routes_turns).reshape((TOKENS, 2))
    keep = draw_keep(jax.random.fold_in(splits[7], 71), 0)
    router = bell_draw(splits[3], (D, EXPERTS), D ** -0.5, 0.078125, ((0, 16),), jnp.float32)
    w_gate = bell_draw(splits[4], (EXPERTS, D, FFW), D ** -0.5, 0.078125, ((0, 8), (2, 32)))
    w_up = bell_draw(splits[5], (EXPERTS, D, FFW), D ** -0.5, 0.078125, ((0, 8), (2, 32)))
    w_down = gaussian_with(splits[6], (EXPERTS, FFW, D), FFW ** -0.5, 0.125, ((0, 8), (1, 32)), (1, 2, 32, 2.75))
    return {"tokens": tokens, "routes": routes, "keep": keep, "router": router, "w_gate": w_gate, "w_up": w_up, "w_down": w_down}


def slot_numbers(block_routes):
    flat = block_routes.reshape(-1)
    onehot = (flat[:, None] == jnp.arange(EXPERTS, dtype=jnp.int32)[None, :]).astype(jnp.int32)
    before = jnp.cumsum(onehot, axis=0) - onehot
    return jnp.sum(before * onehot, axis=1).reshape(block_routes.shape)


def reference(tokens, routes, keep, router, w_gate, w_up, w_down):
    blocks = N_DP * N_EXPERT
    grouped = routes.reshape(blocks, TOK_DEV, 2)
    slots = jax.vmap(slot_numbers)(grouped)
    block_ids = jnp.arange(blocks, dtype=jnp.int32)[:, None, None]
    positions = (block_ids * CAP + slots).astype(jnp.int32)
    spread = jnp.broadcast_to(tokens.reshape(blocks, TOK_DEV, 1, D), (blocks, TOK_DEV, 2, D)).reshape(-1, D)
    expert_rows = jnp.zeros((EXPERTS, blocks * CAP, D), jnp.bfloat16)
    expert_rows = expert_rows.at[grouped.reshape(-1), positions.reshape(-1)].set(spread)
    parts = N_DP * N_FFN
    width = FFW // parts

    def expert_pass(items):
        rows, gate_w, up_w, down_w = items
        gate = jnp.dot(rows, gate_w, preferred_element_type=jnp.float32)
        up = jnp.dot(rows, up_w, preferred_element_type=jnp.float32)
        hidden = (jax.nn.silu(gate) * up).astype(jnp.bfloat16)
        split_hidden = jnp.transpose(hidden.reshape(rows.shape[0], parts, width), (1, 0, 2))
        split_down = down_w.reshape(parts, width, D)

        def add_block(total, pair):
            block_hidden, block_down = pair
            product = jnp.dot(block_hidden, block_down, preferred_element_type=jnp.float32)
            rounded = lax.optimization_barrier(product.astype(jnp.bfloat16))
            return total + rounded.astype(jnp.float32), None

        total, _ = lax.scan(add_block, jnp.zeros((rows.shape[0], D), jnp.float32), (split_hidden, split_down))
        return total.astype(jnp.bfloat16)

    expert_out = lax.map(expert_pass, (expert_rows, w_gate, w_up, w_down))
    flat_pos = positions.reshape(TOKENS, 2)
    first = expert_out[routes[:, 0], flat_pos[:, 0]].astype(jnp.float32)
    second = expert_out[routes[:, 1], flat_pos[:, 1]].astype(jnp.float32)
    logits = jnp.dot(tokens.astype(jnp.float32), router, precision=lax.Precision.HIGHEST)
    logit_first = jnp.take_along_axis(logits, routes[:, 0:1], axis=1)[:, 0]
    logit_second = jnp.take_along_axis(logits, routes[:, 1:2], axis=1)[:, 0]
    keep_f = keep.astype(jnp.float32)
    token_block = (jnp.arange(TOKENS, dtype=jnp.int32) // TOK_DEV).astype(jnp.int32)
    keep_first = keep_f[token_block, routes[:, 0]]
    keep_second = keep_f[token_block, routes[:, 1]]
    diff = logit_first - logit_second
    share = jax.nn.sigmoid(diff)
    other = jax.nn.sigmoid(-diff)
    pruned_first = keep_first * (keep_second * share + 1.0 - keep_second)
    pruned_second = keep_second * (keep_first * other + 1.0 - keep_first)
    full32 = share[:, None] * first + other[:, None] * second
    pruned32 = pruned_first[:, None] * first + pruned_second[:, None] * second
    residual = full32 - pruned32
    inner = jnp.sum(residual * (first - second), axis=1)
    slope = share * (1.0 - share) * (1.0 - keep_first * keep_second) * inner
    expert_ids = jnp.arange(EXPERTS, dtype=jnp.int32)[None, :]
    onehot_first = (routes[:, 0:1] == expert_ids).astype(jnp.float32)
    onehot_second = (routes[:, 1:2] == expert_ids).astype(jnp.float32)
    grad_logits = onehot_first * slope[:, None] - onehot_second * slope[:, None]
    router_grad = jnp.dot(tokens.astype(jnp.float32).T, grad_logits, precision=lax.Precision.HIGHEST)
    return full32.astype(jnp.bfloat16), pruned32.astype(jnp.bfloat16), residual, router_grad
```

```python
import functools

import jax
import jax.numpy as jnp
from jax import lax
from jax.experimental import pallas as pl
from jax.experimental.pallas import tpu as pltpu
from jax.sharding import PartitionSpec as P

MESH = pl.DeviceIdType.MESH
RING = 4
PLANE = RING * RING
HIGH = lax.Precision.HIGHEST


def kernel(
    nz, rows, cols, hid, tok_hbm, routes_hbm, keep_hbm, router_hbm, wg_hbm, wu_hbm, wd_hbm,
    full_hbm, pruned_hbm, resid_hbm, grad_hbm,
    tok, routes, keep, router, wg, wu, wd,
    X, lhs, T, Q, R0, RA1, RA2, RB1, RB2, out, ret,
    LD, LI, LG, stat, full_v, pruned_v, resid_v, grad_v,
    in_sem, out_sem, zin_sem, s1_sem, s1h_sem, s2_sem, s2h_sem, xx_sem, pp_sem,
    a1_sem, a2_sem, b1_sem, b2_sem, ret_sem, small_sem,
    send_ag, send_rs, send_x, send_p, send_z, send_r, send_small,
):
    f32, bf16 = jnp.float32, jnp.bfloat16
    d = lax.axis_index("dp")
    z = lax.axis_index("expert")
    f = lax.axis_index("ffn")
    y, x = f // RING, f % RING
    half = rows // 2
    toks = 2 * rows
    nq = 2 * nz
    me = d * nz + z

    m1, m2 = 1 + (RING - 1) * d, RING - (RING - 1) * d
    c1, c2 = x + d * (y - x), y + d * (x - y)

    def place(a1, a2):
        return ((c1 + a1) % RING) * m1 + ((c2 + a2) % RING) * m2

    up1, dn1, up2, dn2 = place(1, 0), place(3, 0), place(0, 1), place(0, 3)

    def send(src, dst, ssem, rsem, dev):
        pltpu.make_async_remote_copy(
            src_ref=src, dst_ref=dst, send_sem=ssem, recv_sem=rsem, device_id=dev, device_id_type=MESH
        ).start()

    def landed(ref, sem):
        pltpu.make_async_remote_copy(
            src_ref=ref, dst_ref=ref, send_sem=sem, recv_sem=sem, device_id={"ffn": up1}, device_id_type=MESH
        ).wait_recv()

    def sent(ref, sem):
        pltpu.make_async_remote_copy(
            src_ref=ref, dst_ref=ref, send_sem=sem, recv_sem=sem, device_id={"ffn": up1}, device_id_type=MESH
        ).wait_send()

    def plane(p):
        return {"ffn": p}

    barrier = pltpu.get_barrier_semaphore()
    for j in range(1, PLANE):
        pl.semaphore_signal(barrier, inc=1, device_id={"ffn": (f + j) % PLANE}, device_id_type=MESH)
    for j in range(1, nq):
        q = (me + j) % nq
        pl.semaphore_signal(barrier, inc=1, device_id={"dp": q // nz, "expert": q % nz}, device_id_type=MESH)

    loads = [
        pltpu.make_async_copy(routes_hbm, routes, in_sem.at[0]),
        pltpu.make_async_copy(tok_hbm, tok, in_sem.at[1]),
        pltpu.make_async_copy(keep_hbm, keep, in_sem.at[2]),
        pltpu.make_async_copy(router_hbm, router, in_sem.at[3]),
        pltpu.make_async_copy(wg_hbm.at[0], wg, in_sem.at[4]),
        pltpu.make_async_copy(wu_hbm.at[0], wu, in_sem.at[5]),
        pltpu.make_async_copy(wd_hbm.at[0], wd, in_sem.at[6]),
    ]
    for load in loads:
        load.start()

    loads[0].wait()
    r0 = routes[0:1, :]
    r1 = routes[1:2, :]
    expert_rows = lax.broadcasted_iota(jnp.int32, (nz, toks), 0)
    oh0 = (expert_rows == r0).astype(f32)
    oh1 = (expert_rows == r1).astype(f32)
    earlier = (
        lax.broadcasted_iota(jnp.int32, (toks, toks), 0) < lax.broadcasted_iota(jnp.int32, (toks, toks), 1)
    ).astype(bf16)
    before = jnp.dot((oh0 + oh1).astype(bf16), earlier, preferred_element_type=f32)
    pos0 = r0.astype(f32) * rows + jnp.sum(before * oh0, axis=0, keepdims=True)
    pos1 = r1.astype(f32) * rows + jnp.sum(before * oh1, axis=0, keepdims=True)

    loads[1].wait()
    slot = lax.broadcasted_iota(jnp.int32, (rows, toks), 0)
    for k in range(nz):
        e = (z + nz - k) % nz
        at = (slot + e * rows).astype(f32)
        pick = jnp.logical_or(at == pos0, at == pos1).astype(f32).astype(bf16)
        picked = jnp.dot(pick, tok[...], preferred_element_type=f32).astype(bf16)
        if k == 0:
            X[0, 0, f] = picked
        else:
            out[k] = picked
    pl.semaphore_wait(barrier, PLANE - 1 + nq - 1)
    for k in range(1, nz):
        send(out.at[k], X.at[0, k, f], send_z.at[k], zin_sem.at[k], {"expert": (z + nz - k) % nz})

    def ag_a(k):
        @pl.when(k > 0)
        def _():
            landed(X.at[0, k, f], zin_sem.at[k])

        own = X.at[0, k, f]
        send(own, own, send_ag.at[k], s1_sem.at[k, 0], plane(up1))
        send(own, own, send_ag.at[k], s1_sem.at[k, 1], plane(dn1))
        send(own, own, send_ag.at[k], s2_sem.at[k, 0, 0], plane(up2))
        send(own, own, send_ag.at[k], s2_sem.at[k, 1, 0], plane(dn2))

    lo, hi = pl.ds(0, half), pl.ds(half, half)

    def across(k, p, r):
        ref = X.at[0, k, p]
        send(ref, ref, send_ag.at[k], s2_sem.at[k, 0, r], plane(up2))
        send(ref, ref, send_ag.at[k], s2_sem.at[k, 1, r], plane(dn2))

    def ag_b(k):
        landed(X.at[0, k, dn1], s1_sem.at[k, 0])
        send(X.at[0, k, dn1, lo], X.at[0, k, dn1, lo], send_ag.at[k], s1h_sem.at[k, 0], plane(up1))
        across(k, dn1, 1)
        landed(X.at[0, k, up1], s1_sem.at[k, 1])
        send(X.at[0, k, up1, hi], X.at[0, k, up1, hi], send_ag.at[k], s1h_sem.at[k, 1], plane(dn1))
        across(k, up1, 2)

    def ag_c(k):
        op1 = place(2, 0)
        landed(X.at[0, k, op1, lo], s1h_sem.at[k, 0])
        landed(X.at[0, k, op1, hi], s1h_sem.at[k, 1])
        across(k, op1, 3)

    turns = (0, 3, 1, 2)

    def ag_d(k):
        for r, a1 in enumerate(turns):
            p = place(a1, 3)
            landed(X.at[0, k, p], s2_sem.at[k, 0, r])
            send(X.at[0, k, p, lo], X.at[0, k, p, lo], send_ag.at[k], s2h_sem.at[k, 0, r], plane(up2))
            p = place(a1, 1)
            landed(X.at[0, k, p], s2_sem.at[k, 1, r])
            send(X.at[0, k, p, hi], X.at[0, k, p, hi], send_ag.at[k], s2h_sem.at[k, 1, r], plane(dn2))

    def ag_e(k):
        for r, a1 in enumerate(turns):
            p = place(a1, 2)
            landed(X.at[0, k, p, lo], s2h_sem.at[k, 0, r])
            landed(X.at[0, k, p, hi], s2h_sem.at[k, 1, r])
        send(X.at[0, k], X.at[1, k], send_x.at[k], xx_sem.at[k], {"dp": 1 - d})

    def work(k):
        landed(X.at[1, k], xx_sem.at[k])
        for c in range(2):
            for s in range(PLANE):
                lhs[c * rows:(c + 1) * rows, s * cols:(s + 1) * cols] = X[c, k, s]
        gate = jnp.dot(lhs[...], wg[...], preferred_element_type=f32)
        up = jnp.dot(lhs[...], wu[...], preferred_element_type=f32)
        hidden = (gate / (1.0 + jnp.exp(-gate)) * up).astype(bf16)
        for s in range(0, PLANE, 2):
            part = jnp.dot(hidden, wd[:, s * cols:(s + 2) * cols], preferred_element_type=f32).astype(bf16)
            for t in range(2):
                T[k, s + t] = part[0:rows, t * cols:(t + 1) * cols]
                Q[k, s + t] = part[rows:, t * cols:(t + 1) * cols]
        send(Q.at[k], R0.at[k], send_p.at[k], pp_sem.at[k], {"dp": 1 - d})

    def rs_1(k):
        landed(R0.at[k], pp_sem.at[k])
        for a2 in (2, 1, 3, 0):
            for a1 in range(RING):
                p = place(a1, a2)
                T[k, p] = T[k, p] + R0[k, p]
            if a2 == 2:
                for a1 in range(RING):
                    p = place(a1, a2)
                    send(T.at[k, p, lo], RA1.at[k, 0, a1], send_rs.at[k], a1_sem.at[k, 0], plane(up2))
                    send(T.at[k, p, hi], RA1.at[k, 1, a1], send_rs.at[k], a1_sem.at[k, 1], plane(dn2))

    def rs_2(k):
        landed(RA1.at[k, 0], a1_sem.at[k, 0])
        for a1 in range(RING):
            p = place(a1, 1)
            T[k, p, lo] = T[k, p, lo] + RA1[k, 0, a1]
        for a1 in range(RING):
            send(T.at[k, place(a1, 1)], RA2.at[k, 0, a1], send_rs.at[k], a2_sem.at[k, 0], plane(up2))
        landed(RA1.at[k, 1], a1_sem.at[k, 1])
        for a1 in range(RING):
            p = place(a1, 3)
            T[k, p, hi] = T[k, p, hi] + RA1[k, 1, a1]
        for a1 in range(RING):
            send(T.at[k, place(a1, 3)], RA2.at[k, 1, a1], send_rs.at[k], a2_sem.at[k, 1], plane(dn2))

    def total(own, one, two):
        return (own.astype(f32) + one.astype(f32) + two.astype(f32)).astype(bf16)

    def rs_3(k):
        landed(RA2.at[k, 0], a2_sem.at[k, 0])
        landed(RA2.at[k, 1], a2_sem.at[k, 1])
        for a1 in (2, 1, 3, 0):
            p = place(a1, 0)
            T[k, p] = total(T[k, p], RA2[k, 0, a1], RA2[k, 1, a1])
            if a1 == 2:
                send(T.at[k, p, lo], RB1.at[k, 0], send_rs.at[k], b1_sem.at[k, 0], plane(up1))
                send(T.at[k, p, hi], RB1.at[k, 1], send_rs.at[k], b1_sem.at[k, 1], plane(dn1))

    def rs_4(k):
        landed(RB1.at[k, 0], b1_sem.at[k, 0])
        T[k, up1, lo] = T[k, up1, lo] + RB1[k, 0]
        send(T.at[k, up1], RB2.at[k, 0], send_rs.at[k], b2_sem.at[k, 0], plane(up1))
        landed(RB1.at[k, 1], b1_sem.at[k, 1])
        T[k, dn1, hi] = T[k, dn1, hi] + RB1[k, 1]
        send(T.at[k, dn1], RB2.at[k, 1], send_rs.at[k], b2_sem.at[k, 1], plane(dn1))

    def rs_5(k):
        landed(RB2.at[k, 0], b2_sem.at[k, 0])
        landed(RB2.at[k, 1], b2_sem.at[k, 1])
        summed = total(T[k, f], RB2[k, 0], RB2[k, 1])

        @pl.when(k == 0)
        def _():
            ret[z] = summed

        @pl.when(k > 0)
        def _():
            T[k, f] = summed
            send(T.at[k, f], ret.at[z], send_r.at[k], ret_sem.at[k], {"expert": (z + k) % nz})

    def logits_out():
        loads[3].wait()
        local = lax.dot_general(
            router[...], tok[...].astype(f32), (((1,), (1,)), ((), ())), precision=HIGH, preferred_element_type=f32
        )
        part = jnp.sum(local * (oh0 - oh1), axis=0, keepdims=True)
        LD[f] = jnp.broadcast_to(part, (8, toks))
        for j in range(1, PLANE):
            send(LD.at[f], LD.at[f], send_small.at[0], small_sem.at[0], plane((f + j) % PLANE))

    def when(k, stage):
        @pl.when(jnp.logical_and(k >= 0, k < nz))
        def _():
            stage(k)

    @pl.loop(0, nz + 9)
    def _(i):
        when(i, ag_a)
        when(i - 1, ag_b)
        when(i - 2, ag_c)
        when(i - 2, ag_d)
        when(i - 3, ag_e)

        @pl.when(i == 1)
        def _():
            logits_out()

        @pl.when(i == 4)
        def _():
            loads[4].wait()
            loads[5].wait()
            loads[6].wait()

        when(i - 4, work)
        when(i - 5, rs_1)
        when(i - 6, rs_2)
        when(i - 7, rs_3)
        when(i - 8, rs_4)
        when(i - 9, rs_5)

    loads[2].wait()
    landed(LD.at[pl.ds(0, PLANE - 1)], small_sem.at[0])
    diff = jnp.sum(LD[...], axis=0)[0:1]
    wide = jnp.broadcast_to(keep[...].astype(f32), (nz, nz))
    diagonal = lax.broadcasted_iota(jnp.int32, (nz, nz), 0) == lax.broadcasted_iota(jnp.int32, (nz, nz), 1)
    keep_column = jnp.sum(jnp.where(diagonal, wide, 0.0), axis=1, keepdims=True)
    keep0 = jnp.sum(keep_column * oh0, axis=0, keepdims=True)
    keep1 = jnp.sum(keep_column * oh1, axis=0, keepdims=True)
    stat[...] = jnp.zeros_like(stat)
    for j, row in enumerate((pos0, pos1, diff, keep0, keep1)):
        stat[j:j + 1, :] = row
    columns = jnp.transpose(stat[...])
    p0, p1, dc, k0, k1 = (columns[:, j:j + 1] for j in range(5))
    slots = lax.broadcasted_iota(jnp.int32, (toks, nz * rows), 1).astype(f32)
    pick0 = (slots == p0).astype(f32).astype(bf16)
    pick1 = (slots == p1).astype(f32).astype(bf16)
    share, other = 1.0 / (1.0 + jnp.exp(-dc)), 1.0 / (1.0 + jnp.exp(dc))
    pruned0 = k0 * (k1 * share + 1.0 - k1)
    pruned1 = k1 * (k0 * other + 1.0 - k0)

    for k in range(1, nz):
        landed(ret.at[k], ret_sem.at[k])
    returned = ret[...].reshape(nz * rows, cols)
    first = jnp.dot(pick0, returned, preferred_element_type=f32)
    second = jnp.dot(pick1, returned, preferred_element_type=f32)
    full32 = share * first + other * second
    pruned32 = pruned0 * first + pruned1 * second
    residual = full32 - pruned32
    inner_part = jnp.sum(residual * (first - second), axis=1, keepdims=True)
    LI[f] = jnp.transpose(jnp.broadcast_to(inner_part, (toks, 128)))[0:8]
    for j in range(1, PLANE):
        send(LI.at[f], LI.at[f], send_small.at[1], small_sem.at[1], plane((f + j) % PLANE))
    full_v[...] = full32.astype(bf16)
    pruned_v[...] = pruned32.astype(bf16)
    resid_v[...] = residual
    stores = [
        pltpu.make_async_copy(full_v, full_hbm, out_sem.at[0]),
        pltpu.make_async_copy(pruned_v, pruned_hbm, out_sem.at[1]),
        pltpu.make_async_copy(resid_v, resid_hbm, out_sem.at[2]),
    ]
    for store in stores:
        store.start()
    share_row = 1.0 / (1.0 + jnp.exp(-diff))
    rate = share_row * (1.0 - share_row) * (1.0 - keep0 * keep1)
    landed(LI.at[pl.ds(0, PLANE - 1)], small_sem.at[1])
    inner = jnp.sum(LI[...], axis=0)[0:1]
    slope = rate * inner
    LG[me] = jnp.dot(
        (oh0 - oh1) * slope, tok[...].astype(f32), precision=HIGH, preferred_element_type=f32
    )
    for j in range(1, nq):
        q = (me + j) % nq
        send(LG.at[me], LG.at[me], send_small.at[2], small_sem.at[2], {"dp": q // nz, "expert": q % nz})
    landed(LG.at[pl.ds(0, nq - 1)], small_sem.at[2])
    grad_v[...] = jnp.sum(LG[...], axis=0)
    last = pltpu.make_async_copy(grad_v, grad_hbm, out_sem.at[3])
    last.start()

    sent(LD.at[pl.ds(0, PLANE - 1)], send_small.at[0])
    sent(LI.at[pl.ds(0, PLANE - 1)], send_small.at[1])
    sent(LG.at[pl.ds(0, nq - 1)], send_small.at[2])

    @pl.loop(0, nz)
    def _(k):
        sent(X.at[0, k, pl.ds(0, 15)], send_ag.at[k])
        sent(T.at[k, pl.ds(0, 15)], send_rs.at[k])
        sent(X.at[0, k], send_x.at[k])
        sent(Q.at[k], send_p.at[k])

    for k in range(1, nz):
        sent(out.at[k], send_z.at[k])
        sent(T.at[k, f], send_r.at[k])
    for store in stores:
        store.wait()
    last.wait()


def layer(nz, tokens, routes, keep, router, w_gate, w_up, w_down):
    toks, cols = tokens.shape
    rows = toks // 2
    depth, hid = w_gate.shape[1:]
    bf16, f32 = jnp.bfloat16, jnp.float32
    vmem, dma = pltpu.VMEM, pltpu.SemaphoreType.DMA
    shard = (rows, cols)
    piece = (rows // 2, cols)
    nq = 2 * nz
    anywhere = pl.BlockSpec(memory_space=pl.ANY)
    out = pl.pallas_call(
        functools.partial(kernel, nz, rows, cols, hid),
        out_shape=(
            jax.ShapeDtypeStruct((toks, cols), bf16),
            jax.ShapeDtypeStruct((toks, cols), bf16),
            jax.ShapeDtypeStruct((toks, cols), f32),
            jax.ShapeDtypeStruct((nz, cols), f32),
        ),
        in_specs=[anywhere] * 7,
        out_specs=(anywhere,) * 4,
        scratch_shapes=[
            vmem((toks, cols), bf16), vmem((2, toks), jnp.int32), vmem((1, nz), jnp.int32), vmem((nz, cols), f32),
            vmem((depth, hid), bf16), vmem((depth, hid), bf16), vmem((hid, depth), bf16),
            vmem((2, nz, PLANE, *shard), bf16), vmem((toks, depth), bf16),
            vmem((nz, PLANE, *shard), bf16), vmem((nz, PLANE, *shard), bf16), vmem((nz, PLANE, *shard), bf16),
            vmem((nz, 2, RING, *piece), bf16), vmem((nz, 2, RING, *shard), bf16),
            vmem((nz, 2, *piece), bf16), vmem((nz, 2, *shard), bf16),
            vmem((nz, *shard), bf16), vmem((nz, *shard), bf16),
            vmem((PLANE, 8, toks), f32), vmem((PLANE, 8, toks), f32), vmem((nq, nz, cols), f32),
            vmem((128, toks), f32),
            vmem((toks, cols), bf16), vmem((toks, cols), bf16), vmem((toks, cols), f32), vmem((nz, cols), f32),
            dma((7,)), dma((4,)), dma((nz,)), dma((nz, 2)), dma((nz, 2)), dma((nz, 2, RING)), dma((nz, 2, RING)),
            dma((nz,)), dma((nz,)),
            dma((nz, 2)), dma((nz, 2)), dma((nz, 2)), dma((nz, 2)), dma((nz,)), dma((3,)),
            dma((nz,)), dma((nz,)), dma((nz,)), dma((nz,)), dma((nz,)), dma((nz,)), dma((3,)),
        ],
        compiler_params=pltpu.CompilerParams(
            collective_id=0, has_side_effects=True, vmem_limit_bytes=60 * 1024 * 1024
        ),
        name="layer",
    )(tokens, routes.T, keep, router.T, w_gate, w_up, w_down)
    return out[0], out[1], out[2], out[3].T


def solution(mesh):
    return jax.shard_map(
        functools.partial(layer, mesh.shape["expert"]),
        mesh=mesh,
        in_specs=(
            P(("dp", "expert"), "ffn"),
            P(("dp", "expert"), None),
            P(("dp", "expert"), None),
            P("ffn", None),
            P("expert", None, ("dp", "ffn")),
            P("expert", None, ("dp", "ffn")),
            P("expert", ("dp", "ffn"), None),
        ),
        out_specs=(
            P(("dp", "expert"), "ffn"),
            P(("dp", "expert"), "ffn"),
            P(("dp", "expert"), "ffn"),
            P("ffn", None),
        ),
        check_vma=False,
    )
```

```python
import functools

import jax
import jax.numpy as jnp
from jax import lax
from jax.experimental import pallas as pl
from jax.experimental.pallas import tpu as pltpu
from jax.sharding import PartitionSpec as P

MESH = pl.DeviceIdType.MESH
RING = 4
PLANE = RING * RING
HIGH = lax.Precision.HIGHEST
LAG = 6


def kernel(
    nz, rows, cols, hid, tok_hbm, routes_hbm, keep_hbm, router_hbm, wg_hbm, wu_hbm, wd_hbm,
    full_v, pruned_v, resid_v, grad_v,
    tok, routes, keep, router, wg, wu, wd,
    X, lhs, T, Q, R0, RA1, RA2, RB1, RB2, out, ret,
    LD, LI, LG, stat,
    in_sem, zin_sem, s1_sem, s1h_sem, s2_sem, s2h_sem, xx_sem, pp_sem,
    a1_sem, a2_sem, b1_sem, b2_sem, ret_sem, small_sem,
    send_ag, send_rs, send_x, send_p, send_z, send_r, send_small,
):
    f32, bf16 = jnp.float32, jnp.bfloat16
    d = lax.axis_index("dp")
    z = lax.axis_index("expert")
    f = lax.axis_index("ffn")
    y, x = f // RING, f % RING
    half = rows // 2
    toks = 2 * rows
    nq = 2 * nz
    me = d * nz + z

    m1, m2 = 1 + (RING - 1) * d, RING - (RING - 1) * d
    c1, c2 = x + d * (y - x), y + d * (x - y)

    def place(a1, a2):
        return ((c1 + a1) % RING) * m1 + ((c2 + a2) % RING) * m2

    up1, dn1, up2, dn2 = place(1, 0), place(3, 0), place(0, 1), place(0, 3)

    def send(src, dst, ssem, rsem, dev):
        pltpu.make_async_remote_copy(
            src_ref=src, dst_ref=dst, send_sem=ssem, recv_sem=rsem, device_id=dev, device_id_type=MESH
        ).start()

    def landed(ref, sem):
        pltpu.make_async_remote_copy(
            src_ref=ref, dst_ref=ref, send_sem=sem, recv_sem=sem, device_id={"ffn": up1}, device_id_type=MESH
        ).wait_recv()

    def sent(ref, sem):
        pltpu.make_async_remote_copy(
            src_ref=ref, dst_ref=ref, send_sem=sem, recv_sem=sem, device_id={"ffn": up1}, device_id_type=MESH
        ).wait_send()

    def plane(p):
        return {"ffn": p}

    barrier = pltpu.get_barrier_semaphore()
    for j in range(1, PLANE):
        pl.semaphore_signal(barrier, inc=1, device_id={"ffn": (f + j) % PLANE}, device_id_type=MESH)
    for j in range(1, nq):
        q = (me + j) % nq
        pl.semaphore_signal(barrier, inc=1, device_id={"dp": q // nz, "expert": q % nz}, device_id_type=MESH)

    loads = [
        pltpu.make_async_copy(routes_hbm, routes, in_sem.at[0]),
        pltpu.make_async_copy(tok_hbm, tok, in_sem.at[1]),
        pltpu.make_async_copy(keep_hbm, keep, in_sem.at[2]),
        pltpu.make_async_copy(router_hbm, router, in_sem.at[3]),
        pltpu.make_async_copy(wg_hbm.at[0], wg, in_sem.at[4]),
        pltpu.make_async_copy(wu_hbm.at[0], wu, in_sem.at[5]),
        pltpu.make_async_copy(wd_hbm.at[0], wd, in_sem.at[6]),
    ]
    for load in loads:
        load.start()

    loads[0].wait()
    r0 = routes[0:1, :]
    r1 = routes[1:2, :]
    expert_rows = lax.broadcasted_iota(jnp.int32, (nz, toks), 0)
    oh0 = (expert_rows == r0).astype(f32)
    oh1 = (expert_rows == r1).astype(f32)
    earlier = (
        lax.broadcasted_iota(jnp.int32, (toks, toks), 0) < lax.broadcasted_iota(jnp.int32, (toks, toks), 1)
    ).astype(bf16)
    before = jnp.dot((oh0 + oh1).astype(bf16), earlier, preferred_element_type=f32)
    pos0 = r0.astype(f32) * rows + jnp.sum(before * oh0, axis=0, keepdims=True)
    pos1 = r1.astype(f32) * rows + jnp.sum(before * oh1, axis=0, keepdims=True)

    loads[1].wait()
    slot = lax.broadcasted_iota(jnp.int32, (rows, toks), 0)
    for k in range(nz):
        e = (z + nz - k) % nz
        at = (slot + e * rows).astype(f32)
        pick = jnp.logical_or(at == pos0, at == pos1).astype(f32).astype(bf16)
        picked = jnp.dot(pick, tok[...], preferred_element_type=f32).astype(bf16)
        if k == 0:
            X[0, 0, f] = picked
        else:
            out[k] = picked
    pl.semaphore_wait(barrier, PLANE - 1 + nq - 1)
    for k in range(1, nz):
        send(out.at[k], X.at[0, k, f], send_z.at[k], zin_sem.at[k], {"expert": (z + nz - k) % nz})

    def ag_a(k):
        @pl.when(k > 0)
        def _():
            landed(X.at[0, k, f], zin_sem.at[k])

        own = X.at[0, k, f]
        send(own, own, send_ag.at[k], s1_sem.at[k, 0], plane(up1))
        send(own, own, send_ag.at[k], s1_sem.at[k, 1], plane(dn1))
        send(own, own, send_ag.at[k], s2_sem.at[k, 0, 0], plane(up2))
        send(own, own, send_ag.at[k], s2_sem.at[k, 1, 0], plane(dn2))

    lo, hi = pl.ds(0, half), pl.ds(half, half)

    def across(k, p, r):
        ref = X.at[0, k, p]
        send(ref, ref, send_ag.at[k], s2_sem.at[k, 0, r], plane(up2))
        send(ref, ref, send_ag.at[k], s2_sem.at[k, 1, r], plane(dn2))

    def ag_b(k):
        landed(X.at[0, k, dn1], s1_sem.at[k, 0])
        send(X.at[0, k, dn1, lo], X.at[0, k, dn1, lo], send_ag.at[k], s1h_sem.at[k, 0], plane(up1))
        across(k, dn1, 1)
        landed(X.at[0, k, up1], s1_sem.at[k, 1])
        send(X.at[0, k, up1, hi], X.at[0, k, up1, hi], send_ag.at[k], s1h_sem.at[k, 1], plane(dn1))
        across(k, up1, 2)

    def ag_c(k):
        op1 = place(2, 0)
        landed(X.at[0, k, op1, lo], s1h_sem.at[k, 0])
        landed(X.at[0, k, op1, hi], s1h_sem.at[k, 1])
        across(k, op1, 3)

    turns = (0, 3, 1, 2)

    def ag_d(k, which=(0, 1, 2)):
        for r in which:
            a1 = turns[r]
            p = place(a1, 3)
            landed(X.at[0, k, p], s2_sem.at[k, 0, r])
            send(X.at[0, k, p, lo], X.at[0, k, p, lo], send_ag.at[k], s2h_sem.at[k, 0, r], plane(up2))
            p = place(a1, 1)
            landed(X.at[0, k, p], s2_sem.at[k, 1, r])
            send(X.at[0, k, p, hi], X.at[0, k, p, hi], send_ag.at[k], s2h_sem.at[k, 1, r], plane(dn2))

    def ag_d3(k):
        ag_d(k, (3,))

    def ag_e(k):
        for r, a1 in enumerate(turns):
            p = place(a1, 2)
            landed(X.at[0, k, p, lo], s2h_sem.at[k, 0, r])
            landed(X.at[0, k, p, hi], s2h_sem.at[k, 1, r])
        send(X.at[0, k], X.at[1, k], send_x.at[k], xx_sem.at[k], {"dp": 1 - d})

    def work(k):
        landed(X.at[1, k], xx_sem.at[k])
        for c in range(2):
            for s in range(PLANE):
                lhs[c * rows:(c + 1) * rows, s * cols:(s + 1) * cols] = X[c, k, s]
        gate = jnp.dot(lhs[...], wg[...], preferred_element_type=f32)
        up = jnp.dot(lhs[...], wu[...], preferred_element_type=f32)
        hidden = (gate / (1.0 + jnp.exp(-gate)) * up).astype(bf16)
        for s in range(0, PLANE, 2):
            part = jnp.dot(hidden, wd[:, s * cols:(s + 2) * cols], preferred_element_type=f32).astype(bf16)
            for t in range(2):
                T[k, s + t] = part[0:rows, t * cols:(t + 1) * cols]
                Q[k, s + t] = part[rows:, t * cols:(t + 1) * cols]
        send(Q.at[k], R0.at[k], send_p.at[k], pp_sem.at[k], {"dp": 1 - d})

    order = (2, 1, 3, 0)

    def rs_1(k):
        landed(R0.at[k], pp_sem.at[k])

        def across_1(a1):
            p = place(a1, 2)
            send(T.at[k, p, lo], RA1.at[k, 0, a1], send_rs.at[k], a1_sem.at[k, 0, a1], plane(up2))
            send(T.at[k, p, hi], RA1.at[k, 1, a1], send_rs.at[k], a1_sem.at[k, 1, a1], plane(dn2))

        held = None
        for a2 in (2, 1, 3, 0):
            for a1 in order:
                p = place(a1, a2)
                T[k, p] = T[k, p] + R0[k, p]
                if held is not None:
                    across_1(held)
                held = a1 if a2 == 2 else None

    def rs_2(k):
        held = None
        for a1 in order:
            p, q = place(a1, 1), place(a1, 3)
            landed(RA1.at[k, 0, a1], a1_sem.at[k, 0, a1])
            T[k, p, lo] = T[k, p, lo] + RA1[k, 0, a1]
            if held is not None:
                send(T.at[k, place(held, 3)], RA2.at[k, 1, held], send_rs.at[k], a2_sem.at[k, 1, held], plane(dn2))
            landed(RA1.at[k, 1, a1], a1_sem.at[k, 1, a1])
            T[k, q, hi] = T[k, q, hi] + RA1[k, 1, a1]
            send(T.at[k, p], RA2.at[k, 0, a1], send_rs.at[k], a2_sem.at[k, 0, a1], plane(up2))
            held = a1
        send(T.at[k, place(held, 3)], RA2.at[k, 1, held], send_rs.at[k], a2_sem.at[k, 1, held], plane(dn2))

    def total(own, one, two):
        return (own.astype(f32) + one.astype(f32) + two.astype(f32)).astype(bf16)

    def rs_3(k):
        for a1 in order:
            landed(RA2.at[k, 0, a1], a2_sem.at[k, 0, a1])
            landed(RA2.at[k, 1, a1], a2_sem.at[k, 1, a1])
            p = place(a1, 0)
            T[k, p] = total(T[k, p], RA2[k, 0, a1], RA2[k, 1, a1])
            if a1 == order[0]:
                send(T.at[k, p, lo], RB1.at[k, 0], send_rs.at[k], b1_sem.at[k, 0], plane(up1))
                send(T.at[k, p, hi], RB1.at[k, 1], send_rs.at[k], b1_sem.at[k, 1], plane(dn1))

    def rs_4(k):
        landed(RB1.at[k, 0], b1_sem.at[k, 0])
        T[k, up1, lo] = T[k, up1, lo] + RB1[k, 0]
        send(T.at[k, up1], RB2.at[k, 0], send_rs.at[k], b2_sem.at[k, 0], plane(up1))
        landed(RB1.at[k, 1], b1_sem.at[k, 1])
        T[k, dn1, hi] = T[k, dn1, hi] + RB1[k, 1]
        send(T.at[k, dn1], RB2.at[k, 1], send_rs.at[k], b2_sem.at[k, 1], plane(dn1))

    def rs_5(k):
        landed(RB2.at[k, 0], b2_sem.at[k, 0])
        landed(RB2.at[k, 1], b2_sem.at[k, 1])
        summed = total(T[k, f], RB2[k, 0], RB2[k, 1])

        @pl.when(k == 0)
        def _():
            ret[z] = summed

        @pl.when(k > 0)
        def _():
            T[k, f] = summed
            send(T.at[k, f], ret.at[z], send_r.at[k], ret_sem.at[k], {"expert": (z + k) % nz})

    def logits_out():
        loads[3].wait()
        local = lax.dot_general(
            router[...], tok[...].astype(f32), (((1,), (1,)), ((), ())), precision=HIGH, preferred_element_type=f32
        )
        part = jnp.sum(local * (oh0 - oh1), axis=0, keepdims=True)
        LD[f] = jnp.broadcast_to(part, (8, toks))
        for j in range(1, PLANE):
            send(LD.at[f], LD.at[f], send_small.at[0], small_sem.at[0], plane((f + j) % PLANE))

    def when(k, stage):
        @pl.when(jnp.logical_and(k >= 0, k < nz))
        def _():
            stage(k)

    @pl.loop(0, nz + LAG + 4)
    def _(i):
        when(i - 1, ag_b)
        when(i - 2, ag_c)
        when(i - 2, ag_d)
        when(i - 3, ag_d3)
        when(i - 4, ag_e)
        when(2 * i - 1, ag_a)
        when(2 * i, ag_a)

        @pl.when(i == 1)
        def _():
            logits_out()

        @pl.when(i == 5)
        def _():
            loads[4].wait()
            loads[5].wait()
            loads[6].wait()

        when(i - 5, work)
        when(i - LAG, rs_1)
        when(i - LAG - 1, rs_2)
        when(i - LAG - 2, rs_3)
        when(i - LAG - 3, rs_4)
        when(i - LAG - 4, rs_5)

    loads[2].wait()
    landed(LD.at[pl.ds(0, PLANE - 1)], small_sem.at[0])
    diff = jnp.sum(LD[...], axis=0)[0:1]
    wide = jnp.broadcast_to(keep[...].astype(f32), (nz, nz))
    diagonal = lax.broadcasted_iota(jnp.int32, (nz, nz), 0) == lax.broadcasted_iota(jnp.int32, (nz, nz), 1)
    keep_column = jnp.sum(jnp.where(diagonal, wide, 0.0), axis=1, keepdims=True)
    keep0 = jnp.sum(keep_column * oh0, axis=0, keepdims=True)
    keep1 = jnp.sum(keep_column * oh1, axis=0, keepdims=True)
    stat[...] = jnp.zeros_like(stat)
    for j, row in enumerate((pos0, pos1, diff, keep0, keep1)):
        stat[j:j + 1, :] = row
    columns = jnp.transpose(stat[...])
    p0, p1, dc, k0, k1 = (columns[:, j:j + 1] for j in range(5))
    slots = lax.broadcasted_iota(jnp.int32, (toks, nz * rows), 1).astype(f32)
    pick0 = (slots == p0).astype(f32).astype(bf16)
    pick1 = (slots == p1).astype(f32).astype(bf16)
    share, other = 1.0 / (1.0 + jnp.exp(-dc)), 1.0 / (1.0 + jnp.exp(dc))
    pruned0 = k0 * (k1 * share + 1.0 - k1)
    pruned1 = k1 * (k0 * other + 1.0 - k0)

    for k in range(1, nz):
        landed(ret.at[k], ret_sem.at[k])
    returned = ret[...].reshape(nz * rows, cols)
    first = jnp.dot(pick0, returned, preferred_element_type=f32)
    second = jnp.dot(pick1, returned, preferred_element_type=f32)
    full32 = share * first + other * second
    pruned32 = pruned0 * first + pruned1 * second
    residual = full32 - pruned32
    inner_part = jnp.sum(residual * (first - second), axis=1, keepdims=True)
    LI[f] = jnp.transpose(jnp.broadcast_to(inner_part, (toks, 128)))[0:8]
    for j in range(1, PLANE):
        send(LI.at[f], LI.at[f], send_small.at[1], small_sem.at[1], plane((f + j) % PLANE))
    full_v[...] = full32.astype(bf16)
    pruned_v[...] = pruned32.astype(bf16)
    resid_v[...] = residual
    share_row = 1.0 / (1.0 + jnp.exp(-diff))
    rate = share_row * (1.0 - share_row) * (1.0 - keep0 * keep1)
    sent(LD.at[pl.ds(0, PLANE - 1)], send_small.at[0])
    @pl.loop(0, nz)
    def _(k):
        sent(X.at[0, k, pl.ds(0, 15)], send_ag.at[k])
        sent(T.at[k, pl.ds(0, 15)], send_rs.at[k])
        sent(X.at[0, k], send_x.at[k])
        sent(Q.at[k], send_p.at[k])

    for k in range(1, nz):
        sent(out.at[k], send_z.at[k])
        sent(T.at[k, f], send_r.at[k])
    landed(LI.at[pl.ds(0, PLANE - 1)], small_sem.at[1])
    inner = jnp.sum(LI[...], axis=0)[0:1]
    slope = rate * inner
    LG[me] = jnp.dot(
        (oh0 - oh1) * slope, tok[...].astype(f32), precision=HIGH, preferred_element_type=f32
    ).astype(bf16)
    for j in range(1, nq):
        q = (me + j) % nq
        send(LG.at[me], LG.at[me], send_small.at[2], small_sem.at[2], {"dp": q // nz, "expert": q % nz})
    landed(LG.at[pl.ds(0, nq - 1)], small_sem.at[2])
    grad_v[...] = jnp.sum(LG[...].astype(f32), axis=0)
    sent(LI.at[pl.ds(0, PLANE - 1)], send_small.at[1])
    sent(LG.at[pl.ds(0, nq - 1)], send_small.at[2])


def store(*refs):
    sem = refs[8]
    copies = [pltpu.make_async_copy(refs[j], refs[4 + j], sem.at[j]) for j in range(4)]
    for copy in copies:
        copy.start()
    for copy in copies:
        copy.wait()


def layer(nz, tokens, routes, keep, router, w_gate, w_up, w_down):
    toks, cols = tokens.shape
    rows = toks // 2
    depth, hid = w_gate.shape[1:]
    bf16, f32 = jnp.bfloat16, jnp.float32
    vmem, dma = pltpu.VMEM, pltpu.SemaphoreType.DMA
    shard = (rows, cols)
    piece = (rows // 2, cols)
    nq = 2 * nz
    anywhere = pl.BlockSpec(memory_space=pl.ANY)
    shapes = (((toks, cols), bf16), ((toks, cols), bf16), ((toks, cols), f32), ((nz, cols), f32))
    held = pl.pallas_call(
        functools.partial(kernel, nz, rows, cols, hid),
        out_shape=tuple(vmem(*s) for s in shapes),
        in_specs=[anywhere] * 7,
        out_specs=(pl.BlockSpec(memory_space=vmem),) * 4,
        scratch_shapes=[
            vmem((toks, cols), bf16), vmem((2, toks), jnp.int32), vmem((1, nz), jnp.int32), vmem((nz, cols), f32),
            vmem((depth, hid), bf16), vmem((depth, hid), bf16), vmem((hid, depth), bf16),
            vmem((2, nz, PLANE, *shard), bf16), vmem((toks, depth), bf16),
            vmem((nz, PLANE, *shard), bf16), vmem((nz, PLANE, *shard), bf16), vmem((nz, PLANE, *shard), bf16),
            vmem((nz, 2, RING, *piece), bf16), vmem((nz, 2, RING, *shard), bf16),
            vmem((nz, 2, *piece), bf16), vmem((nz, 2, *shard), bf16),
            vmem((nz, *shard), bf16), vmem((nz, *shard), bf16),
            vmem((PLANE, 8, toks), f32), vmem((PLANE, 8, toks), f32), vmem((nq, nz, cols), bf16),
            vmem((128, toks), f32),
            dma((7,)), dma((nz,)), dma((nz, 2)), dma((nz, 2)), dma((nz, 2, RING)), dma((nz, 2, RING)),
            dma((nz,)), dma((nz,)),
            dma((nz, 2, RING)), dma((nz, 2, RING)), dma((nz, 2)), dma((nz, 2)), dma((nz,)), dma((3,)),
            dma((nz,)), dma((nz,)), dma((nz,)), dma((nz,)), dma((nz,)), dma((nz,)), dma((3,)),
        ],
        compiler_params=pltpu.CompilerParams(
            collective_id=0, has_side_effects=True, vmem_limit_bytes=60 * 1024 * 1024
        ),
        name="layer",
    )(tokens, routes.T, keep, router.T, w_gate, w_up, w_down)
    out = pl.pallas_call(
        store,
        out_shape=tuple(jax.ShapeDtypeStruct(*s) for s in shapes),
        in_specs=[pl.BlockSpec(memory_space=vmem)] * 4,
        out_specs=(anywhere,) * 4,
        scratch_shapes=[dma((4,))],
        name="store",
    )(*(pltpu.with_memory_space_constraint(h, vmem) for h in held))
    return out[0], out[1], out[2], out[3].T


def solution(mesh):
    return jax.shard_map(
        functools.partial(layer, mesh.shape["expert"]),
        mesh=mesh,
        in_specs=(
            P(("dp", "expert"), "ffn"),
            P(("dp", "expert"), None),
            P(("dp", "expert"), None),
            P("ffn", None),
            P("expert", None, ("dp", "ffn")),
            P("expert", None, ("dp", "ffn")),
            P("expert", ("dp", "ffn"), None),
        ),
        out_specs=(
            P(("dp", "expert"), "ffn"),
            P(("dp", "expert"), "ffn"),
            P(("dp", "expert"), "ffn"),
            P("ffn", None),
        ),
        check_vma=False,
    )
```

```python
import functools

import jax
import jax.numpy as jnp
from jax import lax
from jax.experimental import pallas as pl
from jax.experimental.pallas import tpu as pltpu
from jax.sharding import PartitionSpec as P

MESH = pl.DeviceIdType.MESH
RING = 4
PLANE = RING * RING
HIGH = lax.Precision.HIGHEST
LAG = 6


def kernel(
    nz, rows, cols, hid, tok_hbm, routes_hbm, keep_hbm, router_hbm, wg_hbm, wu_hbm, wd_hbm,
    full_v, pruned_v, resid_v, grad_v,
    tok, routes, keep, router, wg, wu, wd,
    X0, X1, YS, lhs, T, Q, R0, RA1, RA2, RB1, RB2, RL, out, ret,
    LD, LI, LG, stat,
        in_sem, zin_sem, zf_sem, s1_sem, s1h_sem, s2_sem, s2h_sem, xx_sem, pp_sem,
    a1_sem, a2_sem, b1_sem, b2_sem, rl_sem, ret_sem, small_sem,
    send_ag, send_ra, send_rb, send_rl, send_x, send_p, send_z, send_zf, send_r, send_small,
):
    f32, bf16 = jnp.float32, jnp.bfloat16
    d = lax.axis_index("dp")
    z = lax.axis_index("expert")
    f = lax.axis_index("ffn")
    y, x = f // RING, f % RING
    half = rows // 2
    toks = 2 * rows
    nq = 2 * nz
    me = d * nz + z

    m1, m2 = 1 + (RING - 1) * d, RING - (RING - 1) * d
    c1, c2 = x + d * (y - x), y + d * (x - y)

    def place(a1, a2):
        return ((c1 + a1) % RING) * m1 + ((c2 + a2) % RING) * m2

    up1, dn1, up2, dn2 = place(1, 0), place(3, 0), place(0, 1), place(0, 3)

    def send(src, dst, ssem, rsem, dev):
        pltpu.make_async_remote_copy(
            src_ref=src, dst_ref=dst, send_sem=ssem, recv_sem=rsem, device_id=dev, device_id_type=MESH
        ).start()

    def landed(ref, sem):
        pltpu.make_async_remote_copy(
            src_ref=ref, dst_ref=ref, send_sem=sem, recv_sem=sem, device_id={"ffn": up1}, device_id_type=MESH
        ).wait_recv()

    def sent(ref, sem):
        pltpu.make_async_remote_copy(
            src_ref=ref, dst_ref=ref, send_sem=sem, recv_sem=sem, device_id={"ffn": up1}, device_id_type=MESH
        ).wait_send()

    def plane(p):
        return {"ffn": p}

    barrier = pltpu.get_barrier_semaphore()
    for j in range(1, PLANE):
        pl.semaphore_signal(barrier, inc=1, device_id={"ffn": (f + j) % PLANE}, device_id_type=MESH)
    for j in range(1, nq):
        q = (me + j) % nq
        pl.semaphore_signal(barrier, inc=1, device_id={"dp": q // nz, "expert": q % nz}, device_id_type=MESH)

    for a1 in range(1, RING):
        for step in (1, nz - 1):
            pl.semaphore_signal(
                barrier, inc=1, device_id={"ffn": place(a1, 0), "expert": (z + step) % nz}, device_id_type=MESH
            )

    loads = [
        pltpu.make_async_copy(routes_hbm, routes, in_sem.at[0]),
        pltpu.make_async_copy(tok_hbm, tok, in_sem.at[1]),
        pltpu.make_async_copy(keep_hbm, keep, in_sem.at[2]),
        pltpu.make_async_copy(router_hbm, router, in_sem.at[3]),
        pltpu.make_async_copy(wg_hbm.at[0], wg, in_sem.at[4]),
        pltpu.make_async_copy(wu_hbm.at[0], wu, in_sem.at[5]),
        pltpu.make_async_copy(wd_hbm.at[0], wd, in_sem.at[6]),
        pltpu.make_async_copy(tok_hbm.at[pl.ds(0, rows)], X0.at[nz, f], in_sem.at[7]),
        pltpu.make_async_copy(tok_hbm.at[pl.ds(rows, rows)], X0.at[nz + 1, f], in_sem.at[8]),
    ]
    for load in loads:
        load.start()

    loads[0].wait()
    r0 = routes[0:1, :]
    r1 = routes[1:2, :]
    expert_rows = lax.broadcasted_iota(jnp.int32, (nz, toks), 0)
    oh0 = (expert_rows == r0).astype(f32)
    oh1 = (expert_rows == r1).astype(f32)
    earlier = (
        lax.broadcasted_iota(jnp.int32, (toks, toks), 0) < lax.broadcasted_iota(jnp.int32, (toks, toks), 1)
    ).astype(bf16)
    before = jnp.dot((oh0 + oh1).astype(bf16), earlier, preferred_element_type=f32)
    pos0 = r0.astype(f32) * rows + jnp.sum(before * oh0, axis=0, keepdims=True)
    pos1 = r1.astype(f32) * rows + jnp.sum(before * oh1, axis=0, keepdims=True)

    loads[1].wait()
    slot = lax.broadcasted_iota(jnp.int32, (rows, toks), 0)

    def picks(e):
        at = (slot + e * rows).astype(f32)
        return jnp.logical_or(at == pos0, at == pos1).astype(f32).astype(bf16)

    def away(c):
        far = jnp.where(c == nz - 2, 1, jnp.where(c == nz - 1, nz - 1, c + 1))
        return jnp.where(c == 0, 0, far)

    for c in range(1, nz - 2):
        out[c] = jnp.dot(picks((z + nz - c - 1) % nz), tok[...], preferred_element_type=f32).astype(bf16)
    loads[7].wait()
    loads[8].wait()
    pl.semaphore_wait(barrier, PLANE - 1 + nq - 1 + 2 * (RING - 1))
    for c in range(1, nz - 2):
        send(out.at[c], X0.at[c, f], send_z, zin_sem.at[c], {"expert": (z + nz - c - 1) % nz})

    def share_own(k, m):
        own = X0.at[k, f]
        send(own, own, send_ag, s1_sem.at[m], plane(up1))
        send(own, own, send_ag, s1_sem.at[m], plane(dn1))
        send(own, own, send_ag, s2_sem.at[m, 0], plane(up2))
        send(own, own, send_ag, s2_sem.at[m, 0], plane(dn2))

    def ag_a(k):
        landed(X0.at[k, f], zin_sem.at[k])
        share_own(k, k)

    lo, hi = pl.ds(0, half), pl.ds(half, half)

    def across(k, m, p, r):
        ref = X0.at[k, p]
        send(ref, ref, send_ag, s2_sem.at[m, r], plane(up2))
        send(ref, ref, send_ag, s2_sem.at[m, r], plane(dn2))

    def ag_b(k, m):
        landed(X0.at[k, pl.ds(0, 2)], s1_sem.at[m])
        send(X0.at[k, dn1, lo], X0.at[k, dn1, lo], send_ag, s1h_sem.at[m], plane(up1))
        send(X0.at[k, up1, hi], X0.at[k, up1, hi], send_ag, s1h_sem.at[m], plane(dn1))
        across(k, m, dn1, 1)
        across(k, m, up1, 1)

    def ag_c(k, m):
        landed(X0.at[k, 0], s1h_sem.at[m])
        across(k, m, place(2, 0), 2)

    def ag_d(k, m, r, turns):
        landed(X0.at[k, pl.ds(0, 2 * len(turns))], s2_sem.at[m, r])
        for a1 in turns:
            p, q = place(a1, 3), place(a1, 1)
            send(X0.at[k, p, lo], X0.at[k, p, lo], send_ag, s2h_sem.at[m], plane(up2))
            send(X0.at[k, q, hi], X0.at[k, q, hi], send_ag, s2h_sem.at[m], plane(dn2))

    def ag_d0(k, m):
        ag_d(k, m, 0, (0,))
        ag_d(k, m, 1, (3, 1))

    def ag_d3(k, m):
        ag_d(k, m, 2, (2,))

    def to_sibling(k):
        send(X0.at[k], X1.at[k], send_x, xx_sem.at[k], {"dp": 1 - d})

    def ag_e(k, m):
        landed(X0.at[k, pl.ds(0, RING)], s2h_sem.at[m])

    def dispatch():
        below, above = (z + nz - 1) % nz, (z + 1) % nz
        pick = jnp.concatenate([picks(z), picks(below), picks(above)], axis=0)
        for s in range(PLANE):
            both = jnp.concatenate([X0[nz, s], X0[nz + 1, s]], axis=0)
            picked = jnp.dot(pick, both, preferred_element_type=f32).astype(bf16)
            X0[0, s] = picked[0:rows]
            YS[0, s] = picked[rows:2 * rows]
            YS[1, s] = picked[2 * rows:]
        send(YS.at[0], X0.at[nz - 2], send_zf, zf_sem.at[0], {"expert": below})
        send(YS.at[1], X0.at[nz - 1], send_zf, zf_sem.at[1], {"expert": above})
        to_sibling(0)

    def work(k):
        landed(X1.at[k], xx_sem.at[k])
        for c, source in enumerate((X0, X1)):
            for s in range(PLANE):
                lhs[c * rows:(c + 1) * rows, s * cols:(s + 1) * cols] = source[k, s]
        gate = jnp.dot(lhs[...], wg[...], preferred_element_type=f32)
        up = jnp.dot(lhs[...], wu[...], preferred_element_type=f32)
        hidden = (gate / (1.0 + jnp.exp(-gate)) * up).astype(bf16)
        for s in range(0, PLANE, 2):
            part = jnp.dot(hidden, wd[:, s * cols:(s + 2) * cols], preferred_element_type=f32).astype(bf16)
            for t in range(2):
                T[k, s + t] = part[0:rows, t * cols:(t + 1) * cols]
                Q[k, s + t] = part[rows:, t * cols:(t + 1) * cols]
        send(Q.at[k], R0.at[k], send_p, pp_sem.at[k], {"dp": 1 - d})

    order = (2, 1, 3, 0)

    def rs_1(k):
        landed(R0.at[k], pp_sem.at[k])

        def across_1(a1):
            p = place(a1, 2)
            g = 0 if a1 == order[0] else 1
            send(T.at[k, p, lo], RA1.at[k, 0, a1], send_ra, a1_sem.at[k, g], plane(up2))
            send(T.at[k, p, hi], RA1.at[k, 1, a1], send_ra, a1_sem.at[k, g], plane(dn2))

        held = None
        for a2 in (2, 1, 3, 0):
            for a1 in order:
                p = place(a1, a2)
                T[k, p] = T[k, p] + R0[k, p]
                if held is not None:
                    across_1(held)
                held = a1 if a2 == 2 else None

    def rs_2(k):
        for g, turns in enumerate((order[:1], order[1:])):
            landed(RA1.at[k, :, pl.ds(0, len(turns))], a1_sem.at[k, g])
            for a1 in turns:
                p, q = place(a1, 1), place(a1, 3)
                T[k, p, lo] = T[k, p, lo] + RA1[k, 0, a1]
                T[k, q, hi] = T[k, q, hi] + RA1[k, 1, a1]
            for a1 in turns:
                send(T.at[k, place(a1, 1)], RA2.at[k, 0, a1], send_ra, a2_sem.at[k, g], plane(up2))
                send(T.at[k, place(a1, 3)], RA2.at[k, 1, a1], send_ra, a2_sem.at[k, g], plane(dn2))

    def total(own, one, two):
        return (own.astype(f32) + one.astype(f32) + two.astype(f32)).astype(bf16)

    def rs_3(k):
        home = (z + away(k)) % nz
        for g, turns in enumerate((order[:1], order[1:])):
            landed(RA2.at[k, :, pl.ds(0, len(turns))], a2_sem.at[k, g])
            for a1 in turns:
                p = place(a1, 0)
                T[k, p] = total(T[k, p], RA2[k, 0, a1], RA2[k, 1, a1])

            @pl.when(k >= nz - 2)
            def _():
                for a1 in turns:
                    p = place(a1, 0)
                    send(T.at[k, p], RL.at[k - (nz - 2), a1], send_rl, rl_sem, {"ffn": p, "expert": home})

            if g == 0:
                @pl.when(k < nz - 2)
                def _():
                    p = place(order[0], 0)
                    send(T.at[k, p, lo], RB1.at[k, 0], send_rb, b1_sem.at[k], plane(up1))
                    send(T.at[k, p, hi], RB1.at[k, 1], send_rb, b1_sem.at[k], plane(dn1))

    def rs_4(k):
        landed(RB1.at[k], b1_sem.at[k])
        T[k, up1, lo] = T[k, up1, lo] + RB1[k, 0]
        T[k, dn1, hi] = T[k, dn1, hi] + RB1[k, 1]
        send(T.at[k, up1], RB2.at[k, 0], send_rb, b2_sem.at[k], plane(up1))
        send(T.at[k, dn1], RB2.at[k, 1], send_rb, b2_sem.at[k], plane(dn1))

    def rs_5(k):
        landed(RB2.at[k], b2_sem.at[k])
        summed = total(T[k, f], RB2[k, 0], RB2[k, 1])

        @pl.when(k == 0)
        def _():
            ret[z] = summed

        @pl.when(k > 0)
        def _():
            T[k, f] = summed
            send(T.at[k, f], ret.at[z], send_r, ret_sem, {"expert": (z + away(k)) % nz})

    def logits_out():
        loads[3].wait()
        local = lax.dot_general(
            router[...], tok[...].astype(f32), (((1,), (1,)), ((), ())), precision=HIGH, preferred_element_type=f32
        )
        part = jnp.sum(local * (oh0 - oh1), axis=0, keepdims=True)
        LD[f] = jnp.broadcast_to(part, (8, toks))
        for j in range(1, PLANE):
            send(LD.at[f], LD.at[f], send_small.at[0], small_sem.at[0], plane((f + j) % PLANE))

    def when(k, stage, end=nz):
        @pl.when(jnp.logical_and(k >= 0, k < end))
        def _():
            stage(k)

    def gather(k, stage):
        @pl.when(k == 0)
        def _():
            for j in range(2):
                stage(nz + j, j * (nz - 2))

        @pl.when(jnp.logical_and(k >= 1, k < nz - 2))
        def _():
            stage(k, k)

    def chunk(k, stage):
        @pl.when(jnp.logical_and(k >= 1, k < nz - 2))
        def _():
            stage(k)

    def ready(k):
        gather(k, ag_e)
        chunk(k, to_sibling)

        @pl.when(k == 0)
        def _():
            dispatch()

        @pl.when(jnp.logical_and(k >= nz - 2, k < nz))
        def _():
            landed(X0.at[k], zf_sem.at[k - nz + 2])
            to_sibling(k)

    for j in range(2):
        share_own(nz + j, j * (nz - 2))

    @pl.loop(1, nz + LAG + 2)
    def _(i):
        gather(jnp.where(i == 2, -1, i - 1), ag_b)
        gather(i - 2, ag_c)
        gather(i - 2, ag_d0)

        @pl.when(i == 2)
        def _():
            ag_b(1, 1)

        gather(i - 3, ag_d3)
        ready(i - 4)
        chunk(2 * i - 1, ag_a)
        chunk(2 * i, ag_a)

        @pl.when(i == 1)
        def _():
            logits_out()

        @pl.when(i == 5)
        def _():
            loads[4].wait()
            loads[5].wait()
            loads[6].wait()

        when(i - 5, work)
        when(i - LAG, rs_1)
        when(i - LAG - 1, rs_2)
        when(i - LAG - 2, rs_3)
        when(i - LAG - 3, rs_4, nz - 2)
        when(i - LAG - 4, rs_5, nz - 2)

    loads[2].wait()
    landed(LD.at[pl.ds(0, PLANE - 1)], small_sem.at[0])
    diff = jnp.sum(LD[...], axis=0)[0:1]
    wide = jnp.broadcast_to(keep[...].astype(f32), (nz, nz))
    diagonal = lax.broadcasted_iota(jnp.int32, (nz, nz), 0) == lax.broadcasted_iota(jnp.int32, (nz, nz), 1)
    keep_column = jnp.sum(jnp.where(diagonal, wide, 0.0), axis=1, keepdims=True)
    keep0 = jnp.sum(keep_column * oh0, axis=0, keepdims=True)
    keep1 = jnp.sum(keep_column * oh1, axis=0, keepdims=True)
    stat[...] = jnp.zeros_like(stat)
    for j, row in enumerate((pos0, pos1, diff, keep0, keep1)):
        stat[j:j + 1, :] = row
    columns = jnp.transpose(stat[...])
    p0, p1, dc, k0, k1 = (columns[:, j:j + 1] for j in range(5))
    slots = lax.broadcasted_iota(jnp.int32, (toks, nz * rows), 1).astype(f32)
    pick0 = (slots == p0).astype(f32).astype(bf16)
    pick1 = (slots == p1).astype(f32).astype(bf16)
    share, other = 1.0 / (1.0 + jnp.exp(-dc)), 1.0 / (1.0 + jnp.exp(dc))
    pruned0 = k0 * (k1 * share + 1.0 - k1)
    pruned1 = k1 * (k0 * other + 1.0 - k0)

    landed(ret.at[pl.ds(0, nz - 3)], ret_sem)
    landed(RL, rl_sem)
    for j, step in enumerate((nz - 1, 1)):
        terms = RL[j].astype(f32)
        ret[(z + step) % nz] = (terms[0] + terms[1] + terms[2] + terms[3]).astype(bf16)
    returned = ret[...].reshape(nz * rows, cols)
    first = jnp.dot(pick0, returned, preferred_element_type=f32)
    second = jnp.dot(pick1, returned, preferred_element_type=f32)
    full32 = share * first + other * second
    pruned32 = pruned0 * first + pruned1 * second
    residual = full32 - pruned32
    inner_part = jnp.sum(residual * (first - second), axis=1, keepdims=True)
    LI[f] = jnp.transpose(jnp.broadcast_to(inner_part, (toks, 128)))[0:8]
    for j in range(1, PLANE):
        send(LI.at[f], LI.at[f], send_small.at[1], small_sem.at[1], plane((f + j) % PLANE))
    full_v[...] = full32.astype(bf16)
    pruned_v[...] = pruned32.astype(bf16)
    resid_v[...] = residual
    share_row = 1.0 / (1.0 + jnp.exp(-diff))
    rate = share_row * (1.0 - share_row) * (1.0 - keep0 * keep1)
    sent(LD.at[pl.ds(0, PLANE - 1)], send_small.at[0])
    sent(X0.at[pl.ds(0, nz - 1), pl.ds(0, PLANE - 1)], send_ag)
    sent(T.at[:, pl.ds(0, 3 * RING)], send_ra)
    sent(T.at[pl.ds(0, nz - 2), pl.ds(0, 3)], send_rb)
    sent(RL, send_rl)
    sent(X1, send_x)
    sent(YS, send_zf)
    sent(Q, send_p)
    sent(out.at[pl.ds(0, nz - 3)], send_z)
    sent(out.at[pl.ds(0, nz - 3)], send_r)
    landed(LI.at[pl.ds(0, PLANE - 1)], small_sem.at[1])
    inner = jnp.sum(LI[...], axis=0)[0:1]
    slope = rate * inner
    LG[me] = jnp.dot(
        (oh0 - oh1) * slope, tok[...].astype(f32), precision=HIGH, preferred_element_type=f32
    ).astype(bf16)
    for j in range(1, nq):
        q = (me + j) % nq
        send(LG.at[me], LG.at[me], send_small.at[2], small_sem.at[2], {"dp": q // nz, "expert": q % nz})
    landed(LG.at[pl.ds(0, nq - 1)], small_sem.at[2])
    grad_v[...] = jnp.sum(LG[...].astype(f32), axis=0)
    sent(LI.at[pl.ds(0, PLANE - 1)], send_small.at[1])
    sent(LG.at[pl.ds(0, nq - 1)], send_small.at[2])


def store(*refs):
    sem = refs[8]
    copies = [pltpu.make_async_copy(refs[j], refs[4 + j], sem.at[j]) for j in range(4)]
    for copy in copies:
        copy.start()
    for copy in copies:
        copy.wait()


def layer(nz, tokens, routes, keep, router, w_gate, w_up, w_down):
    toks, cols = tokens.shape
    rows = toks // 2
    depth, hid = w_gate.shape[1:]
    bf16, f32 = jnp.bfloat16, jnp.float32
    vmem, dma = pltpu.VMEM, pltpu.SemaphoreType.DMA
    shard = (rows, cols)
    piece = (rows // 2, cols)
    nq = 2 * nz
    anywhere = pl.BlockSpec(memory_space=pl.ANY)
    shapes = (((toks, cols), bf16), ((toks, cols), bf16), ((toks, cols), f32), ((nz, cols), f32))
    held = pl.pallas_call(
        functools.partial(kernel, nz, rows, cols, hid),
        out_shape=tuple(vmem(*s) for s in shapes),
        in_specs=[anywhere] * 7,
        out_specs=(pl.BlockSpec(memory_space=vmem),) * 4,
        scratch_shapes=[
            vmem((toks, cols), bf16), vmem((2, toks), jnp.int32), vmem((1, nz), jnp.int32), vmem((nz, cols), f32),
            vmem((depth, hid), bf16), vmem((depth, hid), bf16), vmem((hid, depth), bf16),
            vmem((nz + 2, PLANE, *shard), bf16), vmem((nz, PLANE, *shard), bf16), vmem((2, PLANE, *shard), bf16),
            vmem((toks, depth), bf16),
            vmem((nz, PLANE, *shard), bf16), vmem((nz, PLANE, *shard), bf16), vmem((nz, PLANE, *shard), bf16),
            vmem((nz, 2, RING, *piece), bf16), vmem((nz, 2, RING, *shard), bf16),
            vmem((nz - 2, 2, *piece), bf16), vmem((nz - 2, 2, *shard), bf16), vmem((2, RING, *shard), bf16),
            vmem((nz, *shard), bf16), vmem((nz, *shard), bf16),
            vmem((PLANE, 8, toks), f32), vmem((PLANE, 8, toks), f32), vmem((nq, nz, cols), bf16),
            vmem((128, toks), f32),
            dma((9,)), dma((nz,)), dma((2,)), dma((nz,)), dma((nz,)), dma((nz, 3)), dma((nz,)), dma((nz,)), dma((nz,)),
            dma((nz, 2)), dma((nz, 2)), dma((nz - 2,)), dma((nz - 2,)), dma, dma, dma((3,)),
            dma, dma, dma, dma, dma, dma, dma, dma, dma, dma((3,)),
        ],
        compiler_params=pltpu.CompilerParams(
            collective_id=0, has_side_effects=True, vmem_limit_bytes=60 * 1024 * 1024
        ),
        name="layer",
    )(tokens, routes.T, keep, router.T, w_gate, w_up, w_down)
    out = pl.pallas_call(
        store,
        out_shape=tuple(jax.ShapeDtypeStruct(*s) for s in shapes),
        in_specs=[pl.BlockSpec(memory_space=vmem)] * 4,
        out_specs=(anywhere,) * 4,
        scratch_shapes=[dma((4,))],
        name="store",
    )(*(pltpu.with_memory_space_constraint(h, vmem) for h in held))
    return out[0], out[1], out[2], out[3].T


def solution(mesh):
    return jax.shard_map(
        functools.partial(layer, mesh.shape["expert"]),
        mesh=mesh,
        in_specs=(
            P(("dp", "expert"), "ffn"),
            P(("dp", "expert"), None),
            P(("dp", "expert"), None),
            P("ffn", None),
            P("expert", None, ("dp", "ffn")),
            P("expert", None, ("dp", "ffn")),
            P("expert", ("dp", "ffn"), None),
        ),
        out_specs=(
            P(("dp", "expert"), "ffn"),
            P(("dp", "expert"), "ffn"),
            P(("dp", "expert"), "ffn"),
            P("ffn", None),
        ),
        check_vma=False,
    )
```

```python
import functools

import jax
import jax.numpy as jnp
from jax import lax
from jax.experimental import pallas as pl
from jax.experimental.pallas import tpu as pltpu
from jax.sharding import PartitionSpec as P

MESH = pl.DeviceIdType.MESH
RING = 4
PLANE = RING * RING
HIGH = lax.Precision.HIGHEST
LAG = 6


def kernel(
    nz, rows, cols, hid, tok_hbm, routes_hbm, keep_hbm, router_hbm, wg_hbm, wu_hbm, wd_hbm,
    full_v, pruned_v, resid_v, grad_v,
    tok, routes, keep, router, wg, wu, wd,
    X0, X1, YS, lhs, T, Q, R0, RA1, RA2, RB1, RB2, RL, out, ret,
    LD, LI, LG, stat,
        in_sem, zin_sem, zf_sem, s1_sem, s1h_sem, s2_sem, s2h_sem, xx_sem, pp_sem,
    a1_sem, a2_sem, b1_sem, b2_sem, rl_sem, ret_sem, small_sem,
    send_ag, send_ra, send_rb, send_rl, send_x, send_p, send_z, send_zf, send_r, send_small, hop_sem,
):
    f32, bf16 = jnp.float32, jnp.bfloat16
    d = lax.axis_index("dp")
    z = lax.axis_index("expert")
    f = lax.axis_index("ffn")
    y, x = f // RING, f % RING
    half = rows // 2
    toks = 2 * rows
    nq = 2 * nz
    me = d * nz + z

    m1, m2 = 1 + (RING - 1) * d, RING - (RING - 1) * d
    c1, c2 = x + d * (y - x), y + d * (x - y)

    def place(a1, a2):
        return ((c1 + a1) % RING) * m1 + ((c2 + a2) % RING) * m2

    up1, dn1, up2, dn2 = place(1, 0), place(3, 0), place(0, 1), place(0, 3)

    def send(src, dst, ssem, rsem, dev):
        pltpu.make_async_remote_copy(
            src_ref=src, dst_ref=dst, send_sem=ssem, recv_sem=rsem, device_id=dev, device_id_type=MESH
        ).start()

    def landed(ref, sem):
        pltpu.make_async_remote_copy(
            src_ref=ref, dst_ref=ref, send_sem=sem, recv_sem=sem, device_id={"ffn": up1}, device_id_type=MESH
        ).wait_recv()

    def sent(ref, sem):
        pltpu.make_async_remote_copy(
            src_ref=ref, dst_ref=ref, send_sem=sem, recv_sem=sem, device_id={"ffn": up1}, device_id_type=MESH
        ).wait_send()

    def plane(p):
        return {"ffn": p}

    barrier = pltpu.get_barrier_semaphore()
    above, below = (z + 1) % nz, (z + nz - 1) % nz
    beside = [plane(up1), plane(dn1), plane(up2), plane(dn2), {"dp": 1 - d}, {"expert": above}, {"expert": below}]
    for device in beside:
        pl.semaphore_signal(barrier, inc=1, device_id=device, device_id_type=MESH)

    loads = [
        pltpu.make_async_copy(routes_hbm, routes, in_sem.at[0]),
        pltpu.make_async_copy(tok_hbm, tok, in_sem.at[1]),
        pltpu.make_async_copy(keep_hbm, keep, in_sem.at[2]),
        pltpu.make_async_copy(router_hbm, router, in_sem.at[3]),
        pltpu.make_async_copy(wg_hbm.at[0], wg, in_sem.at[4]),
        pltpu.make_async_copy(wu_hbm.at[0], wu, in_sem.at[5]),
        pltpu.make_async_copy(wd_hbm.at[0], wd, in_sem.at[6]),
        pltpu.make_async_copy(tok_hbm.at[pl.ds(0, rows)], X0.at[nz, f], in_sem.at[7]),
        pltpu.make_async_copy(tok_hbm.at[pl.ds(rows, rows)], X0.at[nz + 1, f], in_sem.at[8]),
    ]
    for j in (0, 7, 8, 1, 2, 3, 4, 5, 6):
        loads[j].start()

    loads[0].wait()
    r0 = routes[0:1, :]
    r1 = routes[1:2, :]
    expert_rows = lax.broadcasted_iota(jnp.int32, (nz, toks), 0)
    oh0 = (expert_rows == r0).astype(f32)
    oh1 = (expert_rows == r1).astype(f32)
    earlier = (
        lax.broadcasted_iota(jnp.int32, (toks, toks), 0) < lax.broadcasted_iota(jnp.int32, (toks, toks), 1)
    ).astype(bf16)
    before = jnp.dot((oh0 + oh1).astype(bf16), earlier, preferred_element_type=f32)
    pos0 = r0.astype(f32) * rows + jnp.sum(before * oh0, axis=0, keepdims=True)
    pos1 = r1.astype(f32) * rows + jnp.sum(before * oh1, axis=0, keepdims=True)

    loads[1].wait()
    slot = lax.broadcasted_iota(jnp.int32, (rows, toks), 0)

    def picks(e):
        at = (slot + e * rows).astype(f32)
        return jnp.logical_or(at == pos0, at == pos1).astype(f32).astype(bf16)

    def away(c):
        return jnp.where(c == 0, 0, c + 1)

    for c in range(1, nz - 2):
        out[c] = jnp.dot(picks((z + nz - c - 1) % nz), tok[...], preferred_element_type=f32).astype(bf16)
    def share_own(k, m):
        own = X0.at[k, f]
        send(own, own, send_ag, s1_sem.at[m], plane(up1))
        send(own, own, send_ag, s1_sem.at[m], plane(dn1))
        send(own, own, send_ag, s2_sem.at[m, 0], plane(up2))
        send(own, own, send_ag, s2_sem.at[m, 0], plane(dn2))

    def ag_a(k):
        landed(X0.at[k, f], zin_sem.at[k])
        share_own(k, k)

    lo, hi = pl.ds(0, half), pl.ds(half, half)

    def across(k, m, p, r):
        ref = X0.at[k, p]
        send(ref, ref, send_ag, s2_sem.at[m, r], plane(up2))
        send(ref, ref, send_ag, s2_sem.at[m, r], plane(dn2))

    def ag_b(k, m):
        landed(X0.at[k, pl.ds(0, 2)], s1_sem.at[m])
        send(X0.at[k, dn1, lo], X0.at[k, dn1, lo], send_ag, s1h_sem.at[m], plane(up1))
        send(X0.at[k, up1, hi], X0.at[k, up1, hi], send_ag, s1h_sem.at[m], plane(dn1))
        across(k, m, dn1, 1)
        across(k, m, up1, 1)

    def ag_c(k, m):
        landed(X0.at[k, 0], s1h_sem.at[m])
        across(k, m, place(2, 0), 2)

    def ag_d(k, m, r, turns):
        landed(X0.at[k, pl.ds(0, 2 * len(turns))], s2_sem.at[m, r])
        for a1 in turns:
            p, q = place(a1, 3), place(a1, 1)
            send(X0.at[k, p, lo], X0.at[k, p, lo], send_ag, s2h_sem.at[m], plane(up2))
            send(X0.at[k, q, hi], X0.at[k, q, hi], send_ag, s2h_sem.at[m], plane(dn2))

    def ag_d0(k, m):
        ag_d(k, m, 0, (0,))
        ag_d(k, m, 1, (3, 1))

    def ag_d3(k, m):
        ag_d(k, m, 2, (2,))

    def to_sibling(k):
        send(X0.at[k], X1.at[k], send_x, xx_sem.at[k], {"dp": 1 - d})

    def ag_e(k, m):
        landed(X0.at[k, pl.ds(0, RING)], s2h_sem.at[m])

    def dispatch():
        pick = jnp.concatenate([picks(z), picks(below), picks(above)], axis=0)
        for s in range(PLANE):
            both = jnp.concatenate([X0[nz, s], X0[nz + 1, s]], axis=0)
            picked = jnp.dot(pick, both, preferred_element_type=f32).astype(bf16)
            X0[0, s] = picked[0:rows]
            YS[0, s] = picked[rows:2 * rows]
            YS[1, s] = picked[2 * rows:]
        for j, part in enumerate((lo, hi)):
            send(YS.at[0, :, part], X0.at[nz - 2 + j, :, lo], send_zf, zf_sem.at[j], {"expert": below})
            send(YS.at[1, :, part], X0.at[nz - 2 + j, :, hi], send_zf, zf_sem.at[j], {"expert": above})
        to_sibling(0)

    def work(k):
        landed(X1.at[k], xx_sem.at[k])
        for c, source in enumerate((X0, X1)):
            for s in range(PLANE):
                lhs[c * rows:(c + 1) * rows, s * cols:(s + 1) * cols] = source[k, s]
        gate = jnp.dot(lhs[...], wg[...], preferred_element_type=f32)
        up = jnp.dot(lhs[...], wu[...], preferred_element_type=f32)
        hidden = (gate / (1.0 + jnp.exp(-gate)) * up).astype(bf16)
        for s in range(0, PLANE, 2):
            part = jnp.dot(hidden, wd[:, s * cols:(s + 2) * cols], preferred_element_type=f32).astype(bf16)
            for t in range(2):
                T[k, s + t] = part[0:rows, t * cols:(t + 1) * cols]
                Q[k, s + t] = part[rows:, t * cols:(t + 1) * cols]
        send(Q.at[k], R0.at[k], send_p, pp_sem.at[k], {"dp": 1 - d})

    order = (2, 1, 3, 0)

    def rs_1(k):
        landed(R0.at[k], pp_sem.at[k])

        def across_1(a1):
            p = place(a1, 2)
            g = 0 if a1 == order[0] else 1
            send(T.at[k, p, lo], RA1.at[k, 0, a1], send_ra, a1_sem.at[k, g], plane(up2))
            send(T.at[k, p, hi], RA1.at[k, 1, a1], send_ra, a1_sem.at[k, g], plane(dn2))

        held = None
        for a2 in (2, 1, 3, 0):
            for a1 in order:
                p = place(a1, a2)
                T[k, p] = T[k, p] + R0[k, p]
                if held is not None:
                    across_1(held)
                held = a1 if a2 == 2 else None

    def rs_2(k):
        for g, turns in enumerate((order[:1], order[1:])):
            landed(RA1.at[k, :, pl.ds(0, len(turns))], a1_sem.at[k, g])
            for a1 in turns:
                p, q = place(a1, 1), place(a1, 3)
                T[k, p, lo] = T[k, p, lo] + RA1[k, 0, a1]
                T[k, q, hi] = T[k, q, hi] + RA1[k, 1, a1]
            for a1 in turns:
                send(T.at[k, place(a1, 1)], RA2.at[k, 0, a1], send_ra, a2_sem.at[k, g], plane(up2))
                send(T.at[k, place(a1, 3)], RA2.at[k, 1, a1], send_ra, a2_sem.at[k, g], plane(dn2))

    def total(own, one, two):
        return (own.astype(f32) + one.astype(f32) + two.astype(f32)).astype(bf16)

    def rs_3(k):
        for g, turns in enumerate((order[:1], order[1:])):
            landed(RA2.at[k, :, pl.ds(0, len(turns))], a2_sem.at[k, g])
            for a1 in turns:
                p = place(a1, 0)
                T[k, p] = total(T[k, p], RA2[k, 0, a1], RA2[k, 1, a1])

            @pl.when(k >= nz - 2)
            def _():
                for a1 in turns:
                    p = place(a1, 0)
                    send(T.at[k, p, lo], RL.at[0, k - (nz - 2), a1], send_rl, rl_sem, {"ffn": p, "expert": above})
                    send(T.at[k, p, hi], RL.at[1, k - (nz - 2), a1], send_rl, rl_sem, {"ffn": p, "expert": below})

            if g == 0:
                @pl.when(k < nz - 2)
                def _():
                    p = place(order[0], 0)
                    send(T.at[k, p, lo], RB1.at[k, 0], send_rb, b1_sem.at[k], plane(up1))
                    send(T.at[k, p, hi], RB1.at[k, 1], send_rb, b1_sem.at[k], plane(dn1))

    def rs_4(k):
        landed(RB1.at[k], b1_sem.at[k])
        T[k, up1, lo] = T[k, up1, lo] + RB1[k, 0]
        T[k, dn1, hi] = T[k, dn1, hi] + RB1[k, 1]
        send(T.at[k, up1], RB2.at[k, 0], send_rb, b2_sem.at[k], plane(up1))
        send(T.at[k, dn1], RB2.at[k, 1], send_rb, b2_sem.at[k], plane(dn1))

    def rs_5(k):
        landed(RB2.at[k], b2_sem.at[k])
        summed = total(T[k, f], RB2[k, 0], RB2[k, 1])

        @pl.when(k == 0)
        def _():
            ret[z] = summed

        @pl.when(k > 0)
        def _():
            T[k, f] = summed
            send(T.at[k, f], ret.at[z], send_r, ret_sem, {"expert": (z + away(k)) % nz})

    def logits_out():
        loads[3].wait()
        local = lax.dot_general(
            router[...], tok[...].astype(f32), (((1,), (1,)), ((), ())), precision=HIGH, preferred_element_type=f32
        )
        part = jnp.sum(local * (oh0 - oh1), axis=0, keepdims=True)
        LD[f] = part
        for j in range(1, PLANE):
            send(LD.at[f], LD.at[f], send_small.at[0], small_sem.at[0], plane((f + j) % PLANE))

    def when(k, stage, end=nz):
        @pl.when(jnp.logical_and(k >= 0, k < end))
        def _():
            stage(k)

    def gather(k, stage):
        @pl.when(k == 0)
        def _():
            for j in range(2):
                stage(nz + j, j * (nz - 2))

        @pl.when(jnp.logical_and(k >= 1, k < nz - 2))
        def _():
            stage(k, k)

    def chunk(k, stage):
        @pl.when(jnp.logical_and(k >= 1, k < nz - 2))
        def _():
            stage(k)

    def ready(k):
        gather(k, ag_e)
        chunk(k, to_sibling)

        @pl.when(k == 0)
        def _():
            dispatch()

        @pl.when(jnp.logical_and(k >= nz - 2, k < nz))
        def _():
            landed(X0.at[k], zf_sem.at[k - nz + 2])
            to_sibling(k)

    loads[7].wait()
    loads[8].wait()
    pl.semaphore_wait(barrier, len(beside))
    for j in range(2):
        share_own(nz + j, j * (nz - 2))

    for reach in range(2, nz // 2 + 1):
        for step in (above, below):
            pl.semaphore_signal(hop_sem.at[reach - 2], inc=1, device_id={"expert": step}, device_id_type=MESH)
        pl.semaphore_wait(hop_sem.at[reach - 2], 2)
        for c in sorted({reach - 1, nz - reach - 1}):
            send(out.at[c], X0.at[c, f], send_z, zin_sem.at[c], {"expert": (z + nz - c - 1) % nz})

    @pl.loop(1, nz + LAG + 2)
    def _(i):
        gather(jnp.where(i == 2, -1, i - 1), ag_b)
        gather(i - 2, ag_c)
        gather(i - 2, ag_d0)

        @pl.when(i == 2)
        def _():
            ag_b(1, 1)

        gather(i - 3, ag_d3)
        ready(i - 4)
        chunk(2 * i - 1, ag_a)
        chunk(2 * i, ag_a)

        @pl.when(i == 5)
        def _():
            logits_out()
            loads[4].wait()
            loads[5].wait()
            loads[6].wait()

        when(i - 5, work)
        when(i - LAG, rs_1)
        when(i - LAG - 1, rs_2)
        when(i - LAG - 2, rs_3)
        when(i - LAG - 3, rs_4, nz - 2)
        when(i - LAG - 4, rs_5, nz - 2)

    loads[2].wait()
    landed(LD.at[pl.ds(0, PLANE - 1)], small_sem.at[0])
    diff = jnp.sum(LD[...], axis=0)
    wide = jnp.broadcast_to(keep[...].astype(f32), (nz, nz))
    diagonal = lax.broadcasted_iota(jnp.int32, (nz, nz), 0) == lax.broadcasted_iota(jnp.int32, (nz, nz), 1)
    keep_column = jnp.sum(jnp.where(diagonal, wide, 0.0), axis=1, keepdims=True)
    keep0 = jnp.sum(keep_column * oh0, axis=0, keepdims=True)
    keep1 = jnp.sum(keep_column * oh1, axis=0, keepdims=True)
    stat[...] = jnp.zeros_like(stat)
    for j, row in enumerate((pos0, pos1, diff, keep0, keep1)):
        stat[j:j + 1, :] = row
    columns = jnp.transpose(stat[...])
    p0, p1, dc, k0, k1 = (columns[:, j:j + 1] for j in range(5))
    slots = lax.broadcasted_iota(jnp.int32, (toks, nz * rows), 1).astype(f32)
    pick0 = (slots == p0).astype(f32).astype(bf16)
    pick1 = (slots == p1).astype(f32).astype(bf16)
    share, other = 1.0 / (1.0 + jnp.exp(-dc)), 1.0 / (1.0 + jnp.exp(dc))
    pruned0 = k0 * (k1 * share + 1.0 - k1)
    pruned1 = k1 * (k0 * other + 1.0 - k0)

    landed(ret.at[pl.ds(0, nz - 3)], ret_sem)
    landed(RL, rl_sem)
    for j, step in enumerate((nz - 1, 1)):
        for h in range(2):
            terms = RL[j, h].astype(f32)
            ret[(z + step) % nz, h * half:(h + 1) * half] = (terms[0] + terms[1] + terms[2] + terms[3]).astype(bf16)
    returned = ret[...].reshape(nz * rows, cols)
    first = jnp.dot(pick0, returned, preferred_element_type=f32)
    second = jnp.dot(pick1, returned, preferred_element_type=f32)
    full32 = share * first + other * second
    pruned32 = pruned0 * first + pruned1 * second
    residual = full32 - pruned32
    inner_part = jnp.sum(residual * (first - second), axis=1, keepdims=True)
    LI[f] = jnp.transpose(jnp.broadcast_to(inner_part, (toks, 128)))[0:1]
    for j in range(1, PLANE):
        send(LI.at[f], LI.at[f], send_small.at[1], small_sem.at[1], plane((f + j) % PLANE))
    full_v[...] = full32.astype(bf16)
    pruned_v[...] = pruned32.astype(bf16)
    resid_v[...] = residual
    share_row = 1.0 / (1.0 + jnp.exp(-diff))
    rate = share_row * (1.0 - share_row) * (1.0 - keep0 * keep1)
    sent(LD.at[pl.ds(0, PLANE - 1)], send_small.at[0])
    sent(X0.at[pl.ds(0, nz - 1), pl.ds(0, PLANE - 1)], send_ag)
    sent(T.at[:, pl.ds(0, 3 * RING)], send_ra)
    sent(T.at[pl.ds(0, nz - 2), pl.ds(0, 3)], send_rb)
    sent(RL, send_rl)
    sent(X1, send_x)
    sent(YS, send_zf)
    sent(Q, send_p)
    sent(out.at[pl.ds(0, nz - 3)], send_z)
    sent(out.at[pl.ds(0, nz - 3)], send_r)
    landed(LI.at[pl.ds(0, PLANE - 1)], small_sem.at[1])
    inner = jnp.sum(LI[...], axis=0)
    slope = rate * inner
    LG[me] = jnp.dot(
        (oh0 - oh1) * slope, tok[...].astype(f32), precision=HIGH, preferred_element_type=f32
    ).astype(bf16)
    for j in range(1, nq):
        q = (me + j) % nq
        send(LG.at[me], LG.at[me], send_small.at[2], small_sem.at[2], {"dp": q // nz, "expert": q % nz})
    landed(LG.at[pl.ds(0, nq - 1)], small_sem.at[2])
    grad_v[...] = jnp.sum(LG[...].astype(f32), axis=0)
    sent(LI.at[pl.ds(0, PLANE - 1)], send_small.at[1])
    sent(LG.at[pl.ds(0, nq - 1)], send_small.at[2])


def store(*refs):
    sem = refs[8]
    copies = [pltpu.make_async_copy(refs[j], refs[4 + j], sem.at[j]) for j in range(4)]
    for copy in copies:
        copy.start()
    for copy in copies:
        copy.wait()


def layer(nz, tokens, routes, keep, router, w_gate, w_up, w_down):
    toks, cols = tokens.shape
    rows = toks // 2
    depth, hid = w_gate.shape[1:]
    bf16, f32 = jnp.bfloat16, jnp.float32
    vmem, dma = pltpu.VMEM, pltpu.SemaphoreType.DMA
    shard = (rows, cols)
    piece = (rows // 2, cols)
    nq = 2 * nz
    anywhere = pl.BlockSpec(memory_space=pl.ANY)
    shapes = (((toks, cols), bf16), ((toks, cols), bf16), ((toks, cols), f32), ((nz, cols), f32))
    held = pl.pallas_call(
        functools.partial(kernel, nz, rows, cols, hid),
        out_shape=tuple(vmem(*s) for s in shapes),
        in_specs=[anywhere] * 7,
        out_specs=(pl.BlockSpec(memory_space=vmem),) * 4,
        scratch_shapes=[
            vmem((toks, cols), bf16), vmem((2, toks), jnp.int32), vmem((1, nz), jnp.int32), vmem((nz, cols), f32),
            vmem((depth, hid), bf16), vmem((depth, hid), bf16), vmem((hid, depth), bf16),
            vmem((nz + 2, PLANE, *shard), bf16), vmem((nz, PLANE, *shard), bf16), vmem((2, PLANE, *shard), bf16),
            vmem((toks, depth), bf16),
            vmem((nz, PLANE, *shard), bf16), vmem((nz, PLANE, *shard), bf16), vmem((nz, PLANE, *shard), bf16),
            vmem((nz, 2, RING, *piece), bf16), vmem((nz, 2, RING, *shard), bf16),
            vmem((nz - 2, 2, *piece), bf16), vmem((nz - 2, 2, *shard), bf16), vmem((2, 2, RING, *piece), bf16),
            vmem((nz, *shard), bf16), vmem((nz, *shard), bf16),
            vmem((PLANE, 1, toks), f32), vmem((PLANE, 1, toks), f32), vmem((nq, nz, cols), bf16),
            vmem((128, toks), f32),
            dma((9,)), dma((nz,)), dma((2,)), dma((nz,)), dma((nz,)), dma((nz, 3)), dma((nz,)), dma((nz,)), dma((nz,)),
            dma((nz, 2)), dma((nz, 2)), dma((nz - 2,)), dma((nz - 2,)), dma, dma, dma((3,)),
            dma, dma, dma, dma, dma, dma, dma, dma, dma, dma((3,)), pltpu.SemaphoreType.REGULAR((3,)),
        ],
        compiler_params=pltpu.CompilerParams(
            collective_id=0, has_side_effects=True, vmem_limit_bytes=60 * 1024 * 1024
        ),
        name="layer",
    )(tokens, routes.T, keep, router.T, w_gate, w_up, w_down)
    out = pl.pallas_call(
        store,
        out_shape=tuple(jax.ShapeDtypeStruct(*s) for s in shapes),
        in_specs=[pl.BlockSpec(memory_space=vmem)] * 4,
        out_specs=(anywhere,) * 4,
        scratch_shapes=[dma((4,))],
        name="store",
    )(*(pltpu.with_memory_space_constraint(h, vmem) for h in held))
    return out[0], out[1], out[2], out[3].T


def solution(mesh):
    return jax.shard_map(
        functools.partial(layer, mesh.shape["expert"]),
        mesh=mesh,
        in_specs=(
            P(("dp", "expert"), "ffn"),
            P(("dp", "expert"), None),
            P(("dp", "expert"), None),
            P("ffn", None),
            P("expert", None, ("dp", "ffn")),
            P("expert", None, ("dp", "ffn")),
            P("expert", ("dp", "ffn"), None),
        ),
        out_specs=(
            P(("dp", "expert"), "ffn"),
            P(("dp", "expert"), "ffn"),
            P(("dp", "expert"), "ffn"),
            P("ffn", None),
        ),
        check_vma=False,
    )
```

```python
import functools

import jax
import jax.numpy as jnp
from jax import lax
from jax.experimental import pallas as pl
from jax.experimental.pallas import tpu as pltpu
from jax.sharding import PartitionSpec as P

MESH = pl.DeviceIdType.MESH
RING = 4
PLANE = RING * RING
HIGH = lax.Precision.HIGHEST
LAG = 6


def kernel(
    nz, rows, cols, hid, tok_hbm, routes_hbm, keep_hbm, router_hbm, wg_hbm, wu_hbm, wd_hbm,
    full_v, pruned_v, resid_v, grad_v,
    tok, routes, keep, router, wg, wu, wd,
    X0, X1, YS, lhs, T, Q, R0, RA1, RA2, RB1, RB2, RL, out, ret,
    LD, LI, LG, stat,
        in_sem, zin_sem, zf_sem, s1_sem, s1h_sem, s2_sem, s2h_sem, xx_sem, pp_sem,
    a1_sem, a2_sem, b1_sem, b2_sem, rl_sem, ret_sem, small_sem,
    send_ag, send_ra, send_rb, send_rl, send_x, send_p, send_z, send_zf, send_r, send_small, hop_sem,
):
    f32, bf16 = jnp.float32, jnp.bfloat16
    d = lax.axis_index("dp")
    z = lax.axis_index("expert")
    f = lax.axis_index("ffn")
    y, x = f // RING, f % RING
    half = rows // 2
    toks = 2 * rows
    nq = 2 * nz
    me = d * nz + z

    m1, m2 = 1 + (RING - 1) * d, RING - (RING - 1) * d
    c1, c2 = x + d * (y - x), y + d * (x - y)

    def place(a1, a2):
        return ((c1 + a1) % RING) * m1 + ((c2 + a2) % RING) * m2

    up1, dn1, up2, dn2 = place(1, 0), place(3, 0), place(0, 1), place(0, 3)

    def send(src, dst, ssem, rsem, dev):
        pltpu.make_async_remote_copy(
            src_ref=src, dst_ref=dst, send_sem=ssem, recv_sem=rsem, device_id=dev, device_id_type=MESH
        ).start()

    def landed(ref, sem):
        pltpu.make_async_remote_copy(
            src_ref=ref, dst_ref=ref, send_sem=sem, recv_sem=sem, device_id={"ffn": up1}, device_id_type=MESH
        ).wait_recv()

    def sent(ref, sem):
        pltpu.make_async_remote_copy(
            src_ref=ref, dst_ref=ref, send_sem=sem, recv_sem=sem, device_id={"ffn": up1}, device_id_type=MESH
        ).wait_send()

    def plane(p):
        return {"ffn": p}

    barrier = pltpu.get_barrier_semaphore()
    above, below = (z + 1) % nz, (z + nz - 1) % nz
    beside = [plane(up1), plane(dn1), plane(up2), plane(dn2), {"dp": 1 - d}, {"expert": above}, {"expert": below}]
    for device in beside:
        pl.semaphore_signal(barrier, inc=1, device_id=device, device_id_type=MESH)

    loads = [
        pltpu.make_async_copy(routes_hbm, routes, in_sem.at[0]),
        pltpu.make_async_copy(tok_hbm, tok, in_sem.at[1]),
        pltpu.make_async_copy(keep_hbm, keep, in_sem.at[2]),
        pltpu.make_async_copy(router_hbm, router, in_sem.at[3]),
        pltpu.make_async_copy(wg_hbm.at[0], wg, in_sem.at[4]),
        pltpu.make_async_copy(wu_hbm.at[0], wu, in_sem.at[5]),
        pltpu.make_async_copy(wd_hbm.at[0], wd, in_sem.at[6]),
        pltpu.make_async_copy(tok_hbm.at[pl.ds(0, rows)], X0.at[nz, f], in_sem.at[7]),
        pltpu.make_async_copy(tok_hbm.at[pl.ds(rows, rows)], X0.at[nz + 1, f], in_sem.at[8]),
    ]
    for j in (0, 7, 8, 1, 2, 3, 4, 5, 6):
        loads[j].start()

    loads[0].wait()
    r0 = routes[0:1, :]
    r1 = routes[1:2, :]
    expert_rows = lax.broadcasted_iota(jnp.int32, (nz, toks), 0)
    oh0 = (expert_rows == r0).astype(f32)
    oh1 = (expert_rows == r1).astype(f32)
    earlier = (
        lax.broadcasted_iota(jnp.int32, (toks, toks), 0) < lax.broadcasted_iota(jnp.int32, (toks, toks), 1)
    ).astype(bf16)
    before = jnp.dot((oh0 + oh1).astype(bf16), earlier, preferred_element_type=f32)
    pos0 = r0.astype(f32) * rows + jnp.sum(before * oh0, axis=0, keepdims=True)
    pos1 = r1.astype(f32) * rows + jnp.sum(before * oh1, axis=0, keepdims=True)

    loads[1].wait()
    slot = lax.broadcasted_iota(jnp.int32, (rows, toks), 0)

    def picks(e):
        at = (slot + e * rows).astype(f32)
        return jnp.logical_or(at == pos0, at == pos1).astype(f32).astype(bf16)

    def away(c):
        return jnp.where(c == 0, 0, c + 1)

    for c in range(1, nz - 2):
        out[c] = jnp.dot(picks((z + nz - c - 1) % nz), tok[...], preferred_element_type=f32).astype(bf16)
    def share_own(k, m):
        own = X0.at[k, f]
        send(own, own, send_ag, s1_sem.at[m], plane(up1))
        send(own, own, send_ag, s1_sem.at[m], plane(dn1))
        send(own, own, send_ag, s2_sem.at[m, 0], plane(up2))
        send(own, own, send_ag, s2_sem.at[m, 0], plane(dn2))

    def ag_a(k):
        landed(X0.at[k, f], zin_sem.at[k])
        share_own(k, k)

    lo, hi = pl.ds(0, half), pl.ds(half, half)

    def across(k, m, p, r):
        ref = X0.at[k, p]
        send(ref, ref, send_ag, s2_sem.at[m, r], plane(up2))
        send(ref, ref, send_ag, s2_sem.at[m, r], plane(dn2))

    def ag_b(k, m):
        landed(X0.at[k, pl.ds(0, 2)], s1_sem.at[m])
        send(X0.at[k, dn1, lo], X0.at[k, dn1, lo], send_ag, s1h_sem.at[m], plane(up1))
        send(X0.at[k, up1, hi], X0.at[k, up1, hi], send_ag, s1h_sem.at[m], plane(dn1))
        across(k, m, dn1, 1)
        across(k, m, up1, 1)

    def ag_c(k, m):
        landed(X0.at[k, 0], s1h_sem.at[m])
        across(k, m, place(2, 0), 2)

    def ag_d(k, m, r, turns):
        landed(X0.at[k, pl.ds(0, 2 * len(turns))], s2_sem.at[m, r])
        for a1 in turns:
            p, q = place(a1, 3), place(a1, 1)
            send(X0.at[k, p, lo], X0.at[k, p, lo], send_ag, s2h_sem.at[m], plane(up2))
            send(X0.at[k, q, hi], X0.at[k, q, hi], send_ag, s2h_sem.at[m], plane(dn2))

    def ag_d0(k, m):
        ag_d(k, m, 0, (0,))
        ag_d(k, m, 1, (3, 1))

    def ag_d3(k, m):
        ag_d(k, m, 2, (2,))

    def to_sibling(k):
        send(X0.at[k], X1.at[k], send_x, xx_sem.at[k], {"dp": 1 - d})

    def ag_e(k, m):
        landed(X0.at[k, pl.ds(0, RING)], s2h_sem.at[m])

    def dispatch():
        pick = jnp.concatenate([picks(z), picks(below), picks(above)], axis=0)
        for s in range(PLANE):
            both = jnp.concatenate([X0[nz, s], X0[nz + 1, s]], axis=0)
            picked = jnp.dot(pick, both, preferred_element_type=f32).astype(bf16)
            X0[0, s] = picked[0:rows]
            YS[0, s] = picked[rows:2 * rows]
            YS[1, s] = picked[2 * rows:]
        for j, part in enumerate((lo, hi)):
            send(YS.at[0, :, part], X0.at[nz - 2 + j, :, lo], send_zf, zf_sem.at[j], {"expert": below})
            send(YS.at[1, :, part], X0.at[nz - 2 + j, :, hi], send_zf, zf_sem.at[j], {"expert": above})
        to_sibling(0)

    def work(k):
        landed(X1.at[k], xx_sem.at[k])
        for c, source in enumerate((X0, X1)):
            for s in range(PLANE):
                lhs[c * rows:(c + 1) * rows, s * cols:(s + 1) * cols] = source[k, s]
        gate = jnp.dot(lhs[...], wg[...], preferred_element_type=f32)
        up = jnp.dot(lhs[...], wu[...], preferred_element_type=f32)
        hidden = (gate / (1.0 + jnp.exp(-gate)) * up).astype(bf16)
        for s in range(0, PLANE, 2):
            part = jnp.dot(hidden, wd[:, s * cols:(s + 2) * cols], preferred_element_type=f32).astype(bf16)
            for t in range(2):
                T[k, s + t] = part[0:rows, t * cols:(t + 1) * cols]
                Q[k, s + t] = part[rows:, t * cols:(t + 1) * cols]
        send(Q.at[k], R0.at[k], send_p, pp_sem.at[k], {"dp": 1 - d})

    order = (2, 1, 3, 0)

    def rs_1(k):
        landed(R0.at[k], pp_sem.at[k])

        def across_1(a1):
            p = place(a1, 2)
            g = 0 if a1 == order[0] else 1
            send(T.at[k, p, lo], RA1.at[k, 0, a1], send_ra, a1_sem.at[k, g], plane(up2))
            send(T.at[k, p, hi], RA1.at[k, 1, a1], send_ra, a1_sem.at[k, g], plane(dn2))

        held = None
        for a2 in (2, 1, 3, 0):
            for a1 in order:
                p = place(a1, a2)
                T[k, p] = T[k, p] + R0[k, p]
                if held is not None:
                    across_1(held)
                held = a1 if a2 == 2 else None

    def rs_2(k):
        for g, turns in enumerate((order[:1], order[1:])):
            landed(RA1.at[k, :, pl.ds(0, len(turns))], a1_sem.at[k, g])
            for a1 in turns:
                p, q = place(a1, 1), place(a1, 3)
                T[k, p, lo] = T[k, p, lo] + RA1[k, 0, a1]
                T[k, q, hi] = T[k, q, hi] + RA1[k, 1, a1]
            for a1 in turns:
                send(T.at[k, place(a1, 1)], RA2.at[k, 0, a1], send_ra, a2_sem.at[k, g], plane(up2))
                send(T.at[k, place(a1, 3)], RA2.at[k, 1, a1], send_ra, a2_sem.at[k, g], plane(dn2))

    def total(own, one, two):
        return (own.astype(f32) + one.astype(f32) + two.astype(f32)).astype(bf16)

    def rs_3(k):
        for g, turns in enumerate((order[:1], order[1:])):
            landed(RA2.at[k, :, pl.ds(0, len(turns))], a2_sem.at[k, g])
            for a1 in turns:
                p = place(a1, 0)
                T[k, p] = total(T[k, p], RA2[k, 0, a1], RA2[k, 1, a1])

            @pl.when(k >= nz - 2)
            def _():
                for a1 in turns:
                    p = place(a1, 0)
                    send(T.at[k, p, lo], RL.at[0, k - (nz - 2), a1], send_rl, rl_sem, {"ffn": p, "expert": above})
                    send(T.at[k, p, hi], RL.at[1, k - (nz - 2), a1], send_rl, rl_sem, {"ffn": p, "expert": below})

            if g == 0:
                @pl.when(k < nz - 2)
                def _():
                    p = place(order[0], 0)
                    send(T.at[k, p, lo], RB1.at[k, 0], send_rb, b1_sem.at[k], plane(up1))
                    send(T.at[k, p, hi], RB1.at[k, 1], send_rb, b1_sem.at[k], plane(dn1))

    def rs_4(k):
        landed(RB1.at[k], b1_sem.at[k])
        T[k, up1, lo] = T[k, up1, lo] + RB1[k, 0]
        T[k, dn1, hi] = T[k, dn1, hi] + RB1[k, 1]
        send(T.at[k, up1], RB2.at[k, 0], send_rb, b2_sem.at[k], plane(up1))
        send(T.at[k, dn1], RB2.at[k, 1], send_rb, b2_sem.at[k], plane(dn1))

    def rs_5(k):
        landed(RB2.at[k], b2_sem.at[k])
        summed = total(T[k, f], RB2[k, 0], RB2[k, 1])

        @pl.when(k == 0)
        def _():
            ret[z] = summed

        @pl.when(k > 0)
        def _():
            T[k, f] = summed
            send(T.at[k, f], ret.at[z], send_r, ret_sem, {"expert": (z + away(k)) % nz})

    def logits_out():
        loads[3].wait()
        local = lax.dot_general(
            router[...], tok[...].astype(f32), (((1,), (1,)), ((), ())), precision=HIGH, preferred_element_type=f32
        )
        part = jnp.sum(local * (oh0 - oh1), axis=0, keepdims=True)
        LD[f] = part
        for j in range(1, PLANE):
            send(LD.at[f], LD.at[f], send_small.at[0], small_sem.at[0], plane((f + j) % PLANE))

    def when(k, stage, end=nz):
        @pl.when(jnp.logical_and(k >= 0, k < end))
        def _():
            stage(k)

    def gather(k, stage):
        @pl.when(k == 0)
        def _():
            for j in range(2):
                stage(nz + j, j * (nz - 2))

        @pl.when(jnp.logical_and(k >= 1, k < nz - 2))
        def _():
            stage(k, k)

    def chunk(k, stage, *more):
        @pl.when(jnp.logical_and(k >= 1, k < nz - 2))
        def _():
            stage(k, *more)

    def ready(k):
        gather(k, ag_e)
        chunk(k, to_sibling)

        @pl.when(k == 0)
        def _():
            dispatch()

        @pl.when(jnp.logical_and(k >= nz - 2, k < nz))
        def _():
            landed(X0.at[k], zf_sem.at[k - nz + 2])
            to_sibling(k)

    loads[7].wait()
    loads[8].wait()
    pl.semaphore_wait(barrier, len(beside))
    for j in range(2):
        share_own(nz + j, j * (nz - 2))

    for reach in range(2, nz // 2 + 1):
        for step in (above, below):
            pl.semaphore_signal(hop_sem.at[reach - 2], inc=1, device_id={"expert": step}, device_id_type=MESH)
        pl.semaphore_wait(hop_sem.at[reach - 2], 2)
        for c in sorted({reach - 1, nz - reach - 1}):
            send(out.at[c], X0.at[c, f], send_z, zin_sem.at[c], {"expert": (z + nz - c - 1) % nz})
        if reach == 2:
            for j in range(2):
                ag_b(nz + j, j * (nz - 2))

    @pl.loop(1, nz + LAG + 2)
    def _(i):
        chunk(jnp.where(i == 2, -1, i - 1), ag_b, i - 1)
        gather(i - 2, ag_c)
        gather(i - 2, ag_d0)

        @pl.when(i == 2)
        def _():
            ag_b(1, 1)

        gather(i - 3, ag_d3)
        ready(i - 4)
        chunk(2 * i - 2, ag_a)
        chunk(2 * i - 1, ag_a)

        @pl.when(i == 5)
        def _():
            logits_out()
            loads[4].wait()
            loads[5].wait()
            loads[6].wait()

        when(i - LAG, rs_1)
        when(i - 5, work)
        when(i - LAG - 1, rs_2)
        when(i - LAG - 2, rs_3)
        when(i - LAG - 3, rs_4, nz - 2)
        when(i - LAG - 4, rs_5, nz - 2)

    loads[2].wait()
    landed(LD.at[pl.ds(0, PLANE - 1)], small_sem.at[0])
    diff = jnp.sum(LD[...], axis=0)
    wide = jnp.broadcast_to(keep[...].astype(f32), (nz, nz))
    diagonal = lax.broadcasted_iota(jnp.int32, (nz, nz), 0) == lax.broadcasted_iota(jnp.int32, (nz, nz), 1)
    keep_column = jnp.sum(jnp.where(diagonal, wide, 0.0), axis=1, keepdims=True)
    keep0 = jnp.sum(keep_column * oh0, axis=0, keepdims=True)
    keep1 = jnp.sum(keep_column * oh1, axis=0, keepdims=True)
    stat[...] = jnp.zeros_like(stat)
    for j, row in enumerate((pos0, pos1, diff, keep0, keep1)):
        stat[j:j + 1, :] = row
    columns = jnp.transpose(stat[...])
    p0, p1, dc, k0, k1 = (columns[:, j:j + 1] for j in range(5))
    slots = lax.broadcasted_iota(jnp.int32, (toks, nz * rows), 1).astype(f32)
    pick0 = (slots == p0).astype(f32).astype(bf16)
    pick1 = (slots == p1).astype(f32).astype(bf16)
    share, other = 1.0 / (1.0 + jnp.exp(-dc)), 1.0 / (1.0 + jnp.exp(dc))
    pruned0 = k0 * (k1 * share + 1.0 - k1)
    pruned1 = k1 * (k0 * other + 1.0 - k0)

    landed(ret.at[pl.ds(0, nz - 3)], ret_sem)
    landed(RL, rl_sem)
    for j, step in enumerate((nz - 1, 1)):
        for h in range(2):
            terms = RL[j, h].astype(f32)
            ret[(z + step) % nz, h * half:(h + 1) * half] = (terms[0] + terms[1] + terms[2] + terms[3]).astype(bf16)
    returned = ret[...].reshape(nz * rows, cols)
    first = jnp.dot(pick0, returned, preferred_element_type=f32)
    second = jnp.dot(pick1, returned, preferred_element_type=f32)
    full32 = share * first + other * second
    pruned32 = pruned0 * first + pruned1 * second
    residual = full32 - pruned32
    inner_part = jnp.sum(residual * (first - second), axis=1, keepdims=True)
    LI[f] = jnp.transpose(jnp.broadcast_to(inner_part, (toks, 128)))[0:1]
    for j in range(1, PLANE):
        send(LI.at[f], LI.at[f], send_small.at[1], small_sem.at[1], plane((f + j) % PLANE))
    full_v[...] = full32.astype(bf16)
    pruned_v[...] = pruned32.astype(bf16)
    resid_v[...] = residual
    share_row = 1.0 / (1.0 + jnp.exp(-diff))
    rate = share_row * (1.0 - share_row) * (1.0 - keep0 * keep1)
    sent(LD.at[pl.ds(0, PLANE - 1)], send_small.at[0])
    sent(X0.at[pl.ds(0, nz - 1), pl.ds(0, PLANE - 1)], send_ag)
    sent(T.at[:, pl.ds(0, 3 * RING)], send_ra)
    sent(T.at[pl.ds(0, nz - 2), pl.ds(0, 3)], send_rb)
    sent(RL, send_rl)
    sent(X1, send_x)
    sent(YS, send_zf)
    sent(Q, send_p)
    sent(out.at[pl.ds(0, nz - 3)], send_z)
    sent(out.at[pl.ds(0, nz - 3)], send_r)
    landed(LI.at[pl.ds(0, PLANE - 1)], small_sem.at[1])
    inner = jnp.sum(LI[...], axis=0)
    slope = rate * inner
    LG[me] = jnp.dot(
        (oh0 - oh1) * slope, tok[...].astype(f32), precision=HIGH, preferred_element_type=f32
    ).astype(bf16)
    for j in range(1, nq):
        q = (me + j) % nq
        send(LG.at[me], LG.at[me], send_small.at[2], small_sem.at[2], {"dp": q // nz, "expert": q % nz})
    landed(LG.at[pl.ds(0, nq - 1)], small_sem.at[2])
    grad_v[...] = jnp.sum(LG[...].astype(f32), axis=0)
    sent(LI.at[pl.ds(0, PLANE - 1)], send_small.at[1])
    sent(LG.at[pl.ds(0, nq - 1)], send_small.at[2])


def store(*refs):
    sem = refs[8]
    copies = [pltpu.make_async_copy(refs[j], refs[4 + j], sem.at[j]) for j in range(4)]
    for copy in copies:
        copy.start()
    for copy in copies:
        copy.wait()


def layer(nz, tokens, routes, keep, router, w_gate, w_up, w_down):
    toks, cols = tokens.shape
    rows = toks // 2
    depth, hid = w_gate.shape[1:]
    bf16, f32 = jnp.bfloat16, jnp.float32
    vmem, dma = pltpu.VMEM, pltpu.SemaphoreType.DMA
    shard = (rows, cols)
    piece = (rows // 2, cols)
    nq = 2 * nz
    anywhere = pl.BlockSpec(memory_space=pl.ANY)
    shapes = (((toks, cols), bf16), ((toks, cols), bf16), ((toks, cols), f32), ((nz, cols), f32))
    held = pl.pallas_call(
        functools.partial(kernel, nz, rows, cols, hid),
        out_shape=tuple(vmem(*s) for s in shapes),
        in_specs=[anywhere] * 7,
        out_specs=(pl.BlockSpec(memory_space=vmem),) * 4,
        scratch_shapes=[
            vmem((toks, cols), bf16), vmem((2, toks), jnp.int32), vmem((1, nz), jnp.int32), vmem((nz, cols), f32),
            vmem((depth, hid), bf16), vmem((depth, hid), bf16), vmem((hid, depth), bf16),
            vmem((nz + 2, PLANE, *shard), bf16), vmem((nz, PLANE, *shard), bf16), vmem((2, PLANE, *shard), bf16),
            vmem((toks, depth), bf16),
            vmem((nz, PLANE, *shard), bf16), vmem((nz, PLANE, *shard), bf16), vmem((nz, PLANE, *shard), bf16),
            vmem((nz, 2, RING, *piece), bf16), vmem((nz, 2, RING, *shard), bf16),
            vmem((nz - 2, 2, *piece), bf16), vmem((nz - 2, 2, *shard), bf16), vmem((2, 2, RING, *piece), bf16),
            vmem((nz, *shard), bf16), vmem((nz, *shard), bf16),
            vmem((PLANE, 1, toks), f32), vmem((PLANE, 1, toks), f32), vmem((nq, nz, cols), bf16),
            vmem((128, toks), f32),
            dma((9,)), dma((nz,)), dma((2,)), dma((nz,)), dma((nz,)), dma((nz, 3)), dma((nz,)), dma((nz,)), dma((nz,)),
            dma((nz, 2)), dma((nz, 2)), dma((nz - 2,)), dma((nz - 2,)), dma, dma, dma((3,)),
            dma, dma, dma, dma, dma, dma, dma, dma, dma, dma((3,)), pltpu.SemaphoreType.REGULAR((3,)),
        ],
        compiler_params=pltpu.CompilerParams(
            collective_id=0, has_side_effects=True, vmem_limit_bytes=60 * 1024 * 1024
        ),
        name="layer",
    )(tokens, routes.T, keep, router.T, w_gate, w_up, w_down)
    out = pl.pallas_call(
        store,
        out_shape=tuple(jax.ShapeDtypeStruct(*s) for s in shapes),
        in_specs=[pl.BlockSpec(memory_space=vmem)] * 4,
        out_specs=(anywhere,) * 4,
        scratch_shapes=[dma((4,))],
        name="store",
    )(*(pltpu.with_memory_space_constraint(h, vmem) for h in held))
    return out[0], out[1], out[2], out[3].T


def solution(mesh):
    return jax.shard_map(
        functools.partial(layer, mesh.shape["expert"]),
        mesh=mesh,
        in_specs=(
            P(("dp", "expert"), "ffn"),
            P(("dp", "expert"), None),
            P(("dp", "expert"), None),
            P("ffn", None),
            P("expert", None, ("dp", "ffn")),
            P("expert", None, ("dp", "ffn")),
            P("expert", ("dp", "ffn"), None),
        ),
        out_specs=(
            P(("dp", "expert"), "ffn"),
            P(("dp", "expert"), "ffn"),
            P(("dp", "expert"), "ffn"),
            P("ffn", None),
        ),
        check_vma=False,
    )
```
